32 devices in a mesh: dp: 8 (over z, y), mp: 4 (over x, core).
Axes of the slice: x: 2, y: 2, z: 4, core: 2. Of those that a mesh axis runs over, the one named last changes fastest.
Arguments:
- tokens: bfloat16 [8192, 768], P('dp'), may hold values from -6 to 6
- segments: int32 [16, 512], P('dp'), may hold values from 0 to 7, never falling along the last dimension, each value on 1 to 128 neighbouring positions
- logits_in: bfloat16 [16, 12, 512, 512], P('dp', 'mp'), may hold values from -6 to 6
- w_qkv: bfloat16 [768, 3, 768], P('dp', None, 'mp'), may hold values from -0.21875 to 0.21875
- w_out: bfloat16 [768, 768], P('mp', 'dp'), may hold values from -1.75 to 1.75
- w_up: bfloat16 [768, 3072], P('dp', 'mp'), may hold values from -0.21875 to 0.21875
- w_down: bfloat16 [3072, 768], P('mp', 'dp'), may hold values from -0.15625 to 0.15625
- head_bias: bfloat16 [2, 768], P(None, ('mp', 'dp')), may hold values from -3 to 3
- ff_bias: bfloat16 [3072], P(('mp', 'dp')), may hold values from -3 to 3
- norm_gains: bfloat16 [2, 768], P(None, 'dp'), may hold values from 0.25 to 1.75
- shift_biases: bfloat16 [4, 768], P(None, 'dp'), may hold values from -3 to 3
- grad_out: bfloat16 [8192, 768], P('dp'), may hold values from -6 to 6
- grad_logits: bfloat16 [16, 12, 512, 512], P('dp', 'mp'), may hold values from -0.1796875 to 0.1796875
Outputs:
- mixed: bfloat16 [8192, 768], P('dp')
- logits_out: bfloat16 [16, 12, 512, 512], P('dp', 'mp')
- grad_tokens: bfloat16 [8192, 768], P('dp')
- grad_logits_in: bfloat16 [16, 12, 512, 512], P('dp', 'mp')
- g_w_qkv: float32 [768, 3, 768], P('dp', None, 'mp')
- g_w_out: float32 [768, 768], P('mp', 'dp')
- g_w_up: float32 [768, 3072], P('dp', 'mp')
- g_w_down: float32 [3072, 768], P('mp', 'dp')
- g_head_bias: float32 [2, 768], P(None, ('mp', 'dp'))
- g_ff_bias: float32 [3072], P(('mp', 'dp'))
- g_norm_gains: float32 [2, 768], P(None, 'dp')
- g_shift_biases: float32 [4, 768], P(None, 'dp')
The draws below stay inside these ranges and needn't reach their ends.
Inputs may be any that keep to these rules, and one draw needn't show every extreme that they name: `segments`: within a packed row the ids never fall; each id covers at most 128 consecutive positions and some id of each row covers exactly that many; tokens attend only to tokens of their own id.
All inputs are finite; a program needn't handle non-finite values.
Results may differ from the reference program's by a relative error of at most 0.018.
Values may be sent and summed in bfloat16 or wider, within the bound.
A program may use at most 192 MiB of HBM per device.

```python
import math
import jax
import jax.numpy as jnp
import numpy as np
from jax import lax

D = 768
H = 12
HD = 64
FF = 3072
L = 512
SEGS = 8
SEQS = 16
TOKENS = 8192


def strengthened(values, own_key, source, target, blocks, factor):
    owner, partner = [(jnp.arange(values.shape[position]) // (values.shape[position] // blocks)).reshape([-1 if axis == position else 1 for axis in range(values.ndim)]) for position in (source, target)]
    chosen = jax.random.permutation(own_key, blocks)[partner]
    strong = (owner == chosen) | (owner == (partner + blocks // 2) % blocks)
    return jnp.where(strong, factor * values, values)


def levels(rng, shape, shards, low, top_value):
    loudness = 1.0
    for position, blocks in shards:
        draws = jax.random.uniform(jax.random.fold_in(jax.random.fold_in(rng, 6), position), (blocks,), jnp.float32, low / len(shards), top_value / len(shards))
        loudness = loudness * jnp.repeat(jnp.exp(draws), shape[position] // blocks).reshape((-1,) + (1,) * (len(shape) - 1 - position))
    return loudness


def length_profile(number_of, total, bound, skew):
    weights = [(1 << 20) // math.isqrt(standing ** skew) + 1 for standing in range(2, number_of + 1)]
    rest, counts = total - bound - (number_of - 1), [1] * (number_of - 1)
    while rest > 0:
        movable = [i for i in range(number_of - 1) if counts[i] < bound]
        whole, remaining = sum([weights[i] for i in movable]), rest
        for i in movable:
            more = min(bound - counts[i], max(1, remaining * weights[i] // whole), rest)
            counts[i] = counts[i] + more
            rest = rest - more
    return np.array([bound] + counts)


def uneven(stream_key, amount, total, most, lean):
    if amount == 2:
        one = jax.random.randint(stream_key, (), max(1, total - most), min(most, total - 1) + 1)
        return jnp.stack([one, total - one])
    lengths = jnp.asarray(length_profile(amount, total, most, lean), jnp.int32)
    couples = (amount - 1) // 2
    giver, receiver = lengths[1:1 + 2 * couples:2], lengths[2:2 + 2 * couples:2]
    slack = jnp.minimum(giver - 1, most - receiver)
    passed = jax.random.randint(jax.random.fold_in(stream_key, 1), (couples,), 0, 1 << 20) % (slack + 1)
    lengths = lengths.at[1:1 + 2 * couples:2].set(giver - passed).at[2:2 + 2 * couples:2].set(receiver + passed)
    return lengths[jax.random.permutation(jax.random.fold_in(stream_key, 2), amount)]


def noise(own_key, dims, deviation, bound, shards=(), kind=jnp.bfloat16):
    entries = jax.random.normal(own_key, dims, jnp.float32) * deviation
    if len(shards) > 0:
        entries = levels(own_key, dims, shards, -0.22, 0.18) * entries
    return jnp.clip(entries, min=-bound, max=bound).astype(kind)


def bell_draw_with(stream_key, dims, width, bound, cuts, heavy, dtype=jnp.bfloat16):
    entries = width * jax.random.normal(stream_key, dims, jnp.float32)
    if cuts:
        entries = entries * levels(stream_key, dims, cuts, -0.22, 0.18)
    return jnp.clip(strengthened(entries, jax.random.fold_in(stream_key, 3), *heavy), -bound, bound).astype(dtype)


def setup_inputs(seed: int = 0) -> dict:
    streams_of = jax.random.split(jax.random.key(seed), 14)
    return {
        "tokens": bell_draw_with(streams_of[0], (TOKENS, D), 1.0, 6.0, ((0, 8),), (0, 1, 8, 2.0)),
        "segments": jax.vmap(lambda own: jnp.searchsorted(jnp.cumsum(uneven(own, SEGS, L, L // 4, 2)), jnp.arange(L), side="right"))(jax.random.split(streams_of[1], SEQS)).reshape((SEQS, L)).astype(jnp.int32),
        "logits_in": noise(streams_of[2], (SEQS, H, L, L), 1.0, 6.0, ((0, 8), (1, 4))),
        "w_qkv": noise(streams_of[3], (D, 3, D), D ** -0.5, 0.21875, ((0, 8), (2, 4))),
        "w_out": noise(streams_of[4], (D, D), (D * SEGS // L) ** -0.5, 1.75, ((0, 4), (1, 8))),
        "w_up": noise(streams_of[5], (D, FF), D ** -0.5, 0.21875, ((0, 8), (1, 4))),
        "w_down": noise(streams_of[6], (FF, D), (FF // 2) ** -0.5, 0.15625, ((0, 4), (1, 8))),
        "head_bias": noise(streams_of[7], (2, D), 0.5, 3.0, ((1, 32),)),
        "ff_bias": noise(streams_of[8], (FF,), 0.5, 3.0, ((0, 32),)),
        "norm_gains": jnp.clip(1.0 + 0.15 * jax.random.normal(streams_of[9], (2, D), jnp.float32), 0.25, 1.75).astype(jnp.bfloat16),
        "shift_biases": noise(streams_of[10], (4, D), 0.5, 3.0, ((1, 8),)),
        "grad_out": bell_draw_with(streams_of[11], (TOKENS, D), 1.0, 6.0, ((0, 8),), (0, 1, 8, 2.0)),
        "grad_logits": noise(streams_of[12], (SEQS, H, L, L), 0.03, 0.1796875, ((0, 8), (1, 4))),
    }


@jax.custom_vjp
def low(v):
    return lax.optimization_barrier(v.astype(jnp.bfloat16)).astype(jnp.float32)

@jax.custom_vjp
def low_back(v):
    return v

def low_keep(v):
    return (low(v), None)

def low_pass(kept, grad):
    return (grad,)

def back_keep(v):
    return (v, None)

def back_low(kept, grad):
    return (low(grad),)
low.defvjp(low_keep, low_pass)
low_back.defvjp(back_keep, back_low)
epsilon = 1e-05
masked_value = -10000.0
highest = lax.Precision.HIGHEST

def norm_rows(hidden, gain, shift):
    center = hidden - lax.optimization_barrier(jnp.mean(hidden, axis=-1, keepdims=True))
    spread = lax.optimization_barrier(jnp.mean(center * center, axis=-1, keepdims=True))
    return center * lax.rsqrt(spread + epsilon) * gain + shift

def gelu_exact(value):
    return 0.5 * value * (1.0 + lax.erf(value * 0.7071067811865476))

def matmul_high(left, right):
    return jnp.dot(left, right, precision=highest)

def group_layer(weights, block_tokens, block_logits, block_segments):
    qkv_weight, out_weight, up_weight, down_weight, bias_heads, bias_hidden, gains, shifts = weights
    group_size = block_segments.shape[0]
    projected = matmul_high(block_tokens, qkv_weight.reshape(D, 3 * D))
    shape_heads = (group_size, L, H, HD)
    query = low(low_back(projected[:, :D] + bias_heads[0])).reshape(shape_heads)
    keys = low(low_back(projected[:, D:2 * D])).reshape(shape_heads)
    values = low(low_back(projected[:, 2 * D:] + bias_heads[1])).reshape(shape_heads)
    product = jnp.einsum('sqhd,skhd->shqk', query, keys, precision=highest)
    raw = low_back(product * 0.125) + block_logits
    same = block_segments[:, :, None] == block_segments[:, None, :]
    mask = jnp.where(same, 0.0, masked_value)[:, None]
    prob = jax.nn.softmax(raw + mask, axis=-1)
    context = jnp.einsum('shqk,skhd->sqhd', low(prob), values, precision=highest).reshape(group_size * L, D)
    context = low(low_back(context))
    branch = low_back(matmul_high(context, out_weight) + shifts[0])
    normed = low(norm_rows(branch + block_tokens, gains[0], shifts[1]))
    hidden = low_back(matmul_high(normed, up_weight) + bias_hidden)
    activated = low(gelu_exact(hidden))
    second_branch = low_back(matmul_high(activated, down_weight) + shifts[2])
    result = norm_rows(second_branch + normed, gains[1], shifts[3])
    return (result, raw)

def reference(tokens, segments, logits_in, w_qkv, w_out, w_up, w_down, head_bias, ff_bias, norm_gains, shift_biases, grad_out, grad_logits):

    def to_float(array):
        return array.astype(jnp.float32)
    params = (to_float(w_qkv), to_float(w_out), to_float(w_up), to_float(w_down), to_float(head_bias), to_float(ff_bias), to_float(norm_gains), to_float(shift_biases))
    groups = SEQS // 8

    def forward(weights, inputs, incoming):

        def one_group(item):
            return group_layer(weights, item[0], item[1], item[2])
        results, raws = lax.map(jax.checkpoint(one_group), (inputs.reshape(groups, 8 * L, D), incoming.reshape(groups, 8, H, L, L), segments.reshape(groups, 8, L)))
        return (results.reshape(TOKENS, D), raws.reshape(SEQS, H, L, L))
    (mixed, raw), pull = jax.vjp(forward, params, to_float(tokens), to_float(logits_in))
    grads, grad_inputs, grad_incoming = pull((to_float(grad_out), to_float(grad_logits)))
    return (mixed.astype(jnp.bfloat16), raw.astype(jnp.bfloat16), grad_inputs.astype(jnp.bfloat16), grad_incoming.astype(jnp.bfloat16), grads[0], grads[1], grads[2], grads[3], grads[4], grads[5], grads[6], grads[7])
```

```python
import functools

import jax
import jax.numpy as jnp
from jax import lax
from jax.experimental import pallas as pl
from jax.experimental.pallas import tpu as pltpu
from jax.sharding import PartitionSpec as P

MB = 2
MESH = pl.DeviceIdType.MESH
F32 = jnp.float32
BF16 = jnp.bfloat16

epsilon = 1e-05
masked_value = -10000.0


def norm_rows(hidden, gain, shift):
    center = hidden - jnp.mean(hidden, axis=-1, keepdims=True)
    spread = jnp.mean(center * center, axis=-1, keepdims=True)
    return center * lax.rsqrt(spread + epsilon) * gain + shift


def gelu_exact(value):
    return 0.5 * value * (1.0 + lax.erf(value * 0.7071067811865476))


def add_trees(first_tree, second_tree):
    if first_tree is None:
        return second_tree
    return jax.tree.map(jnp.add, first_tree, second_tree)


def micro_step(whole, block_tokens, block_segments, block_logits, block_grad, block_grad_logits):
    qkv_weight, out_weight, up_weight, down_weight, bias_heads, bias_hidden, gains, shifts = whole
    seq_count = block_segments.shape[0]
    length = block_segments.shape[1]
    feature = block_tokens.shape[1]
    row_count = block_tokens.shape[0]
    local_heads = block_logits.shape[1]
    flat_qkv = qkv_weight.reshape(feature, -1)
    local_cols = flat_qkv.shape[1] // 3
    head_size = local_cols // local_heads
    gain_rows = gains.astype(jnp.float32)
    shift_rows = shifts.astype(jnp.float32)
    head_rows = bias_heads.astype(jnp.float32)
    shape_heads = (seq_count, length, local_heads, head_size)
    token_float = block_tokens.astype(jnp.float32)
    projected = jnp.dot(block_tokens, flat_qkv, preferred_element_type=jnp.float32)
    query = (projected[:, :local_cols] + head_rows[0]).astype(jnp.bfloat16).reshape(shape_heads)
    keys = projected[:, local_cols : 2 * local_cols].astype(jnp.bfloat16).reshape(shape_heads)
    values = (
        (projected[:, 2 * local_cols :] + head_rows[1]).astype(jnp.bfloat16).reshape(shape_heads)
    )
    same = block_segments[:, :, None] == block_segments[:, None, :]
    mask = jnp.where(same, 0.0, masked_value).astype(jnp.float32)[:, None]
    incoming = block_logits.astype(jnp.float32)
    raw = (
        jnp.einsum("sqhd,skhd->shqk", query, keys, preferred_element_type=jnp.float32) * 0.125
        + incoming
    )
    shifted = raw + mask
    top = jnp.max(shifted, axis=-1, keepdims=True)
    expo = jnp.exp(shifted - top)
    total = jnp.sum(expo, axis=-1, keepdims=True)
    log_total = top + jnp.log(total)
    context = jnp.einsum(
        "shqk,skhd->sqhd",
        (expo / total).astype(jnp.bfloat16),
        values,
        preferred_element_type=jnp.float32,
    )
    context = context.reshape(row_count, local_cols).astype(jnp.bfloat16)
    attn_total = lax.psum(jnp.dot(context, out_weight, preferred_element_type=jnp.float32), "mp")
    first_pre = attn_total + shift_rows[0] + token_float
    normed = norm_rows(first_pre, gain_rows[0], shift_rows[1]).astype(jnp.bfloat16)
    hidden_pre = jnp.dot(
        normed, up_weight, preferred_element_type=jnp.float32
    ) + bias_hidden.astype(jnp.float32)
    activated = gelu_exact(hidden_pre).astype(jnp.bfloat16)
    ffn_total = lax.psum(jnp.dot(activated, down_weight, preferred_element_type=jnp.float32), "mp")
    second_pre = ffn_total + shift_rows[2] + normed.astype(jnp.float32)
    cotangent = block_grad.astype(jnp.float32)
    mixed_part = norm_rows(second_pre, gain_rows[1], shift_rows[3]).astype(jnp.bfloat16)
    unused_second, second_pull = jax.vjp(norm_rows, second_pre, gain_rows[1], shift_rows[3])
    grad_second, grad_gain_two, grad_shift_two = second_pull(cotangent)
    branch_part = grad_second.astype(jnp.bfloat16)
    grad_bias_two = jnp.sum(branch_part.astype(jnp.float32), axis=0)
    grad_down = jnp.einsum("rf,rd->fd", activated, branch_part, preferred_element_type=jnp.float32)
    grad_act = jnp.einsum("rd,fd->rf", branch_part, down_weight, preferred_element_type=jnp.float32)
    unused_gelu, gelu_pull = jax.vjp(gelu_exact, hidden_pre)
    grad_hidden = gelu_pull(grad_act)[0].astype(jnp.bfloat16)
    grad_bias_hidden = jnp.sum(grad_hidden.astype(jnp.float32), axis=0)
    grad_up = jnp.einsum("rd,rf->df", normed, grad_hidden, preferred_element_type=jnp.float32)
    hidden_terms = jnp.einsum(
        "rf,df->rd", grad_hidden, up_weight, preferred_element_type=jnp.float32
    )
    grad_normed = grad_second + lax.psum(hidden_terms, "mp")
    unused_first, first_pull = jax.vjp(norm_rows, first_pre, gain_rows[0], shift_rows[1])
    grad_first, grad_gain_one, grad_shift_one = first_pull(grad_normed)
    grad_attn = grad_first.astype(jnp.bfloat16)
    grad_bias_out = jnp.sum(grad_attn.astype(jnp.float32), axis=0)
    grad_out_weight = jnp.einsum(
        "rc,rd->cd", context, grad_attn, preferred_element_type=jnp.float32
    )
    grad_context = jnp.einsum(
        "rd,cd->rc", grad_attn, out_weight, preferred_element_type=jnp.float32
    )
    grad_context = grad_context.astype(jnp.bfloat16).reshape(shape_heads)
    raw_again = (
        jnp.einsum("sqhd,skhd->shqk", query, keys, preferred_element_type=jnp.float32) * 0.125
        + incoming
    )
    prob = jnp.exp(raw_again + mask - log_total)
    grad_prob = jnp.einsum(
        "sqhd,skhd->shqk", grad_context, values, preferred_element_type=jnp.float32
    )
    grad_raw = prob * (
        grad_prob - jnp.sum(prob * grad_prob, axis=-1, keepdims=True)
    ) + block_grad_logits.astype(jnp.float32)
    grad_raw_low = grad_raw.astype(jnp.bfloat16)
    grad_query = (
        jnp.einsum("shqk,skhd->sqhd", grad_raw_low, keys, preferred_element_type=jnp.float32)
        * 0.125
    )
    grad_keys = (
        jnp.einsum("shqk,sqhd->skhd", grad_raw_low, query, preferred_element_type=jnp.float32)
        * 0.125
    )
    grad_values = jnp.einsum(
        "shqk,sqhd->skhd",
        prob.astype(jnp.bfloat16),
        grad_context,
        preferred_element_type=jnp.float32,
    )
    grad_query = grad_query.astype(jnp.bfloat16).reshape(row_count, local_cols)
    grad_keys = grad_keys.astype(jnp.bfloat16).reshape(row_count, local_cols)
    grad_values = grad_values.astype(jnp.bfloat16).reshape(row_count, local_cols)
    grad_proj = jnp.concatenate([grad_query, grad_keys, grad_values], axis=1)
    grad_qkv = jnp.einsum(
        "rd,rc->dc", block_tokens, grad_proj, preferred_element_type=jnp.float32
    ).reshape(qkv_weight.shape)
    grad_heads = jnp.stack(
        [
            jnp.sum(grad_query.astype(jnp.float32), axis=0),
            jnp.sum(grad_values.astype(jnp.float32), axis=0),
        ]
    )
    input_terms = jnp.einsum("rc,dc->rd", grad_proj, flat_qkv, preferred_element_type=jnp.float32)
    grad_inputs = grad_first + lax.psum(input_terms.astype(jnp.bfloat16), "mp").astype(jnp.float32)
    results = (mixed_part, raw.astype(jnp.bfloat16), grad_inputs.astype(jnp.bfloat16), grad_raw_low)
    grads = (
        grad_qkv,
        grad_out_weight,
        grad_up,
        grad_down,
        grad_heads,
        grad_bias_hidden,
        jnp.stack([grad_gain_one, grad_gain_two]),
        jnp.stack([grad_bias_out, grad_shift_one, grad_bias_two, grad_shift_two]),
    )
    return (results, grads)


def shards(
    tokens,
    segments,
    logits_in,
    w_qkv,
    w_out,
    w_up,
    w_down,
    head_bias,
    ff_bias,
    norm_gains,
    shift_biases,
    grad_out,
    grad_logits,
):
    seq_count = segments.shape[0] // MB
    row_count = seq_count * segments.shape[1]
    collected = []
    totals = None
    for micro in range(MB):
        whole = (
            lax.all_gather(w_qkv, "dp", axis=0, tiled=True),
            lax.all_gather(w_out, "dp", axis=1, tiled=True),
            lax.all_gather(w_up, "dp", axis=0, tiled=True),
            lax.all_gather(w_down, "dp", axis=1, tiled=True),
            lax.all_gather(head_bias, "dp", axis=1, tiled=True),
            lax.all_gather(ff_bias, "dp", axis=0, tiled=True),
            lax.all_gather(norm_gains, "dp", axis=1, tiled=True),
            lax.all_gather(shift_biases, "dp", axis=1, tiled=True),
        )
        first_row = micro * row_count
        first_seq = micro * seq_count
        results, grads = micro_step(
            whole,
            tokens[first_row : first_row + row_count],
            segments[first_seq : first_seq + seq_count],
            logits_in[first_seq : first_seq + seq_count],
            grad_out[first_row : first_row + row_count],
            grad_logits[first_seq : first_seq + seq_count],
        )
        totals = add_trees(totals, grads)
        collected.append(results)
    totals = (
        lax.psum_scatter(totals[0], "dp", scatter_dimension=0, tiled=True),
        lax.psum_scatter(totals[1], "dp", scatter_dimension=1, tiled=True),
        lax.psum_scatter(totals[2], "dp", scatter_dimension=0, tiled=True),
        lax.psum_scatter(totals[3], "dp", scatter_dimension=1, tiled=True),
        lax.psum_scatter(totals[4], "dp", scatter_dimension=1, tiled=True),
        lax.psum_scatter(totals[5], "dp", scatter_dimension=0, tiled=True),
        lax.psum_scatter(totals[6], "dp", scatter_dimension=1, tiled=True),
        lax.psum_scatter(totals[7], "dp", scatter_dimension=1, tiled=True),
    )
    mixed = jnp.concatenate([item[0] for item in collected], axis=0)
    logits_out = jnp.concatenate([item[1] for item in collected], axis=0)
    grad_tokens = jnp.concatenate([item[2] for item in collected], axis=0)
    grad_logits_in = jnp.concatenate([item[3] for item in collected], axis=0)
    return (
        mixed,
        logits_out,
        grad_tokens,
        grad_logits_in,
        totals[0],
        totals[1],
        totals[2],
        totals[3],
        totals[4],
        totals[5],
        totals[6],
        totals[7],
    )


Z, Y, CORES = 4, 2, 2
TILE = 32
EDGE = 128
CHUNK = 256
COPIES = 96


def dot_nn(a, b):
    return lax.dot_general(a, b, (((1,), (0,)), ((), ())), preferred_element_type=F32)


def dot_nt(a, b):
    return lax.dot_general(a, b, (((1,), (1,)), ((), ())), preferred_element_type=F32)


def dot_tn(a, b):
    return lax.dot_general(a, b, (((0,), (0,)), ((), ())), preferred_element_type=F32)


def fold_rows(value):
    rows, cols = value.shape
    return jnp.sum(value.reshape(rows // 8, 8, cols), axis=0)


class Wires:
    def __init__(self, send_sem, recv_sem):
        self.send_sem, self.recv_sem, self.sent, self.drained = send_sem, recv_sem, [], []

    def send(self, src, dst, device):
        index = len(self.sent)
        copy = pltpu.make_async_remote_copy(
            src_ref=src,
            dst_ref=dst,
            send_sem=self.send_sem.at[index],
            recv_sem=self.recv_sem.at[index],
            device_id=device,
            device_id_type=MESH,
        )
        copy.start()
        self.sent.append(copy)
        return copy

    def drain(self, copy):
        copy.wait_send()
        self.drained.append(copy)

    def drain_all(self):
        for copy in self.sent:
            if not any(copy is done for done in self.drained):
                copy.wait_send()


def layer_kernel(names, dims, *refs):
    r_ = dict(zip(names, refs, strict=True))
    L, HEADS, HD, D, FF, C, SH = dims
    seqs = 2
    half = L // 2
    tok, seg, GOUT = r_["tok"], r_["seg"], r_["GOUT"]
    WA, WU, WD, WO, SMV = r_["WA"], r_["WU"], r_["WD"], r_["WO"], r_["SMV"]
    Q, K, V, LIN, GLB, PROB = r_["Q"], r_["K"], r_["V"], r_["LIN"], r_["GLB"], r_["PROB"]
    BIAS, CTXF, CTXR = r_["BIAS"], r_["CTXF"], r_["CTXR"]
    NORMED, ACT, DG, BR, GH, GAT = r_["NORMED"], r_["ACT"], r_["DG"], r_["BR"], r_["GH"], r_["GAT"]
    GC, MIX, GT, XH1, R1, GS = r_["GC"], r_["MIX"], r_["GT"], r_["XH1"], r_["R1"], r_["GS"]
    HB, CS, CR, XS, XR = r_["HB"], r_["CS"], r_["CR"], r_["XS"], r_["XR"]
    OWN, GP = r_["OWN"], r_["GP"]
    GQF, GKF, GVF = r_["GQF"], r_["GKF"], r_["GVF"]
    SMG, SMS, SMR = r_["SMG"], r_["SMS"], r_["SMR"]
    local_sem = r_["local_sem"]

    dpi, mpi = lax.axis_index("dp"), lax.axis_index("mp")
    z, y = lax.div(dpi, Y), lax.rem(dpi, Y)
    x, core = lax.div(mpi, CORES), lax.rem(mpi, CORES)
    wires = Wires(r_["send_sem"], r_["recv_sem"])

    def dev(zz, yy, xx, cc):
        return {"dp": zz * Y + yy, "mp": xx * CORES + cc}

    zto = [lax.rem(z + k, Z) for k in range(Z)]
    zfrom = [lax.rem(z - k + Z, Z) for k in range(Z)]
    z_dev = [dev(zto[k], y, x, core) for k in range(Z)]
    y_dev = dev(z, 1 - y, x, core)
    c_dev = dev(z, y, x, 1 - core)
    x_dev = dev(z, y, 1 - x, core)
    d_dev = dev(z, y, 1 - x, 1 - core)

    def local(src, dst, index):
        copy = pltpu.make_async_copy(src, dst, local_sem.at[index])
        copy.start()
        return copy

    load_lin = [local(r_["lin"].at[s], LIN.at[s], s) for s in range(seqs)]
    load_gout = [
        local(r_["gout"].at[pl.ds(pl.multiple_of(s * L + core * half, half), half), :], GOUT.at[s], 4 + s)
        for s in range(seqs)
    ]
    load_gl = [local(r_["gl"].at[s], GLB.at[s], 2 + s) for s in range(seqs)]

    barrier = pltpu.get_barrier_semaphore()
    friends = z_dev[1:] + [y_dev, c_dev, x_dev, d_dev]
    for friend in friends:
        pl.semaphore_signal(barrier, inc=1, device_id=friend, device_id_type=MESH)
    pl.semaphore_wait(barrier, len(friends))

    def rows_of(index):
        return pl.ds(pl.multiple_of(index * SH, SH), SH)

    class Gather:
        def __init__(self, src, dst, place):
            self.src, self.dst, self.place = src, dst, place
            self.here = place(z * Y + y)
            self.zs = [wires.send(src, dst.at[self.here], z_dev[k]) for k in range(1, Z)]
            self.ys = [wires.send(src, dst.at[self.here], y_dev)]

        def keep(self):
            self.dst[self.here] = self.src[...]

        def forward(self):
            for k in range(1, Z):
                self.zs[k - 1].wait_recv()
                at = self.place(zfrom[k] * Y + y)
                self.ys.append(wires.send(self.dst.at[at], self.dst.at[at], y_dev))

        def finish(self):
            for copy in self.ys:
                copy.wait_recv()

    def by_rows(index):
        return (rows_of(index), slice(None))

    gather_a = Gather(r_["wa"], WA, lambda i: (slice(None), rows_of(i), slice(None)))
    gather_s = Gather(r_["sm"], r_["SM"], lambda i: (i,))
    gather_u = Gather(r_["wu"], WU, by_rows)
    gather_d = Gather(r_["wd"], WD, by_rows)
    for gather in (gather_a, gather_s, gather_u, gather_d):
        gather.keep()
    gather_a.forward()
    gather_s.forward()
    gather_a.finish()
    gather_s.finish()

    wo_core = wires.send(WA.at[3], WO.at[0], c_dev)
    wo_x = wires.send(WA.at[3], WO.at[1], x_dev)

    summed = r_["SM"][0].astype(F32)
    for i in range(1, Z * Y):
        summed = summed + r_["SM"][i].astype(F32)
    SMV[...] = summed
    SMG[...] = jnp.zeros_like(SMG)

    def vec(row, width=D):
        return SMV[row : row + 1, :width]

    def project(i, carry):
        rows = pl.ds(pl.multiple_of(i * CHUNK, CHUNK), CHUNK)
        block = tok[rows, :]
        Q[rows, :] = (dot_nn(block, WA[0]) + vec(8, C)).astype(BF16)
        K[rows, :] = dot_nn(block, WA[1]).astype(BF16)
        V[rows, :] = (dot_nn(block, WA[2]) + vec(9, C)).astype(BF16)
        return carry

    lax.fori_loop(0, seqs * L // CHUNK, project, 0)

    lanes = lax.broadcasted_iota(jnp.int32, (1, C), 1) // HD

    def head_mask(h):
        return jnp.where(lanes == h, 1.0, 0.0).astype(BF16)

    blocks = L // EDGE
    windows = [(max(b - 1, 0) * EDGE, min(b + 2, blocks) * EDGE) for b in range(blocks)]

    def half_of(s, which):
        return pl.ds(pl.multiple_of(s * L + which * half, half), half)

    def mine(s):
        return half_of(s, core)

    def theirs(s):
        return half_of(s, 1 - core)

    def attend(s):
        base = s * L
        ids = seg[s : s + 1, :].astype(F32)
        tall = jnp.transpose(jnp.broadcast_to(ids, (EDGE, L)))
        for b, (lo, hi) in enumerate(windows):
            for j in range((hi - lo) // EDGE):
                near = ids[:, lo + j * EDGE : lo + (j + 1) * EDGE]
                same = tall[b * EDGE : (b + 1) * EDGE, :] == near
                BIAS[b * EDGE : (b + 1) * EDGE, j * EDGE : (j + 1) * EDGE] = jnp.where(
                    same, 0.0, masked_value
                ).astype(F32)
        GQF[...] = jnp.zeros_like(GQF)
        load_lin[s].wait()

        def head(h, carry):
            pick = head_mask(h)
            for b, (lo, hi) in enumerate(windows):
                rows = slice(b * EDGE, (b + 1) * EDGE)
                query = Q[base + b * EDGE : base + (b + 1) * EDGE, :] * pick
                score = dot_nt(query, K[base : base + L, :])
                raw = score * 0.125 + LIN[s, h, rows, :].astype(F32)
                LIN[s, h, rows, :] = raw.astype(BF16)
                near = raw[:, lo:hi] + BIAS[rows, : hi - lo]
                top = jnp.max(near, axis=-1, keepdims=True)
                expo = jnp.exp(near - top)
                norm = 1.0 / jnp.sum(expo, axis=-1, keepdims=True)
                prob = (expo * norm).astype(BF16)
                PROB[s, h, rows, : hi - lo] = prob
                GQF[rows, :] += dot_nn(prob, V[base + lo : base + hi, :] * pick)
            return carry

        lax.fori_loop(0, HEADS, head, 0)
        CTXF[base : base + L, :] = GQF[...].astype(BF16)
        store = local(LIN.at[s], r_["logits_out"].at[s], s)
        parts = [
            wires.send(CTXF.at[theirs(s), :], CTXR.at[0, s], c_dev),
            wires.send(CTXF.at[mine(s), :], CTXR.at[1, s], x_dev),
            wires.send(CTXF.at[theirs(s), :], CTXR.at[2, s], d_dev),
        ]
        return store, parts

    def tile_loop(count, body, init):
        def step(i, carry):
            return body(pl.multiple_of(i * TILE, TILE), carry)

        return lax.fori_loop(0, count // TILE, step, init)

    def token_rows(s, r):
        return pl.ds(pl.multiple_of(s * L + core * half + r, TILE), TILE)

    def normalize(value):
        center = value - jnp.mean(value, axis=-1, keepdims=True)
        spread = jnp.mean(center * center, axis=-1, keepdims=True)
        scale = lax.rsqrt(spread + epsilon)
        return center * scale, scale

    def norm_back(scaled, xhat, scale):
        flat = jnp.mean(scaled, axis=-1, keepdims=True)
        tilt = jnp.mean(scaled * xhat, axis=-1, keepdims=True)
        return scale * (scaled - flat - xhat * tilt)

    def add_small(rows, sums):
        for row, value in zip(rows, sums, strict=True):
            SMG[row : row + 1, :] += jnp.sum(value, axis=0, keepdims=True)

    def share(ref, s):
        return wires.send(ref.at[mine(s), :], ref.at[mine(s), :], c_dev)

    def out_project(s, parts):
        for copy in parts:
            copy.wait_recv()
        HB[...] = dot_nt(CTXF[mine(s), :], WA[3]) + dot_nt(CTXR[0, s], WO[0])
        HB[...] += dot_nt(CTXR[1, s], WO[1]) + dot_nt(CTXR[2, s], WO[2])

        def body(r, carry):
            at = pl.ds(r, TILE)
            first = HB[at, :] + vec(2) + tok[token_rows(s, r), :].astype(F32)
            xhat, scale = normalize(first)
            XH1[s, at, :] = xhat
            R1[s, at, :] = jnp.broadcast_to(scale, (TILE, EDGE))
            NORMED[token_rows(s, r), :] = (xhat * vec(0) + vec(3)).astype(BF16)
            return carry

        tile_loop(half, body, 0)
        return share(NORMED, s)

    def feed_up(s):
        def block(i, carry):
            start = s * L + i * CHUNK
            rows = pl.ds(pl.multiple_of(start, CHUNK), CHUNK)
            HB[...] = dot_nn(NORMED[rows, :], WU[...]) + vec(10, FF)

            def body(r, inner):
                to = pl.ds(pl.multiple_of(start + r, TILE), TILE)
                value = HB[pl.ds(r, TILE), :]
                cdf = 0.5 * (1.0 + lax.erf(value * 0.7071067811865476))
                ACT[to, :] = (value * cdf).astype(BF16)
                DG[to, :] = cdf + value * (jnp.exp(-0.5 * value * value) * 0.3989422804014327)
                return inner

            return tile_loop(CHUNK, body, carry)

        lax.fori_loop(0, L // CHUNK, block, 0)

    last_sum = [None] * seqs

    class Reduction:
        def __init__(self, stage, s, product):
            self.stage, self.s = stage, s
            before = last_sum[s]
            if before is not None:
                wires.drain(before.pair)
                wires.drain(before.far)
            last_sum[s] = self
            CS[s] = product(theirs(s)).astype(BF16)
            self.pair = wires.send(CS.at[s], CR.at[s], c_dev)
            OWN[s] = product(mine(s))

        def cross(self):
            s = self.s
            self.pair.wait_recv()
            XS[s] = (OWN[s] + CR[s].astype(F32)).astype(BF16)
            self.far = wires.send(XS.at[s], XR.at[self.stage, s], x_dev)

        def wait(self):
            self.far.wait_recv()

        def tile(self, r):
            at = pl.ds(r, TILE)
            return XS[self.s, at, :].astype(F32) + XR[self.stage, self.s, at, :].astype(F32)

    def feed_down(s):
        return Reduction(0, s, lambda rows: dot_nt(ACT[rows, :], WD[...]))

    zeros = jnp.zeros((8, D), F32)

    def norm_two(s, total):
        total.wait()
        load_gout[s].wait()

        def body(r, carry):
            gain, shift, bias = carry
            rows = token_rows(s, r)
            second = total.tile(r) + vec(4) + NORMED[rows, :].astype(F32)
            xhat, scale = normalize(second)
            MIX[rows, :] = (xhat * vec(1) + vec(5)).astype(BF16)
            cot = GOUT[s, pl.ds(r, TILE), :].astype(F32)
            back = norm_back(cot * vec(1), xhat, scale)
            GS[s, pl.ds(r, TILE), :] = back
            low = back.astype(BF16)
            BR[rows, :] = low
            gain = gain + fold_rows(cot * xhat)
            shift = shift + fold_rows(cot)
            bias = bias + fold_rows(low.astype(F32))
            return gain, shift, bias

        add_small((1, 5, 4), tile_loop(half, body, (zeros, zeros, zeros)))
        return share(BR, s), share(MIX, s)

    def feed_back(s):
        def block(i, carry):
            start = s * L + i * CHUNK
            rows = pl.ds(pl.multiple_of(start, CHUNK), CHUNK)
            HB[...] = dot_nn(BR[rows, :], WD[...])

            def body(r, total):
                to = pl.ds(pl.multiple_of(start + r, TILE), TILE)
                low = (HB[pl.ds(r, TILE), :] * DG[to, :]).astype(BF16)
                GH[to, :] = low
                return total + fold_rows(low.astype(F32))

            return tile_loop(CHUNK, body, carry)

        sums = lax.fori_loop(0, L // CHUNK, block, jnp.zeros((8, FF), F32))
        SMG[10:11, :FF] += jnp.sum(sums, axis=0, keepdims=True)
        return Reduction(1, s, lambda rows: dot_nt(GH[rows, :], WU[...]))

    def norm_one_back(s, total):
        total.wait()

        def body(r, carry):
            gain, shift, bias = carry
            at = pl.ds(r, TILE)
            cot = GS[s, at, :] + total.tile(r)
            xhat = XH1[s, at, :]
            back = norm_back(cot * vec(0), xhat, R1[s, at, 0:1])
            GS[s, at, :] = back
            low = back.astype(BF16)
            GAT[token_rows(s, r), :] = low
            gain = gain + fold_rows(cot * xhat)
            shift = shift + fold_rows(cot)
            bias = bias + fold_rows(low.astype(F32))
            return gain, shift, bias

        add_small((0, 3, 2), tile_loop(half, body, (zeros, zeros, zeros)))
        return share(GAT, s)

    def attend_back(s):
        base = s * L
        all_rows = slice(base, base + L)
        GC[...] = dot_nn(GAT[all_rows, :], WA[3]).astype(BF16)
        GQF[...] = jnp.zeros_like(GQF)
        GKF[...] = jnp.zeros_like(GKF)
        GVF[...] = jnp.zeros_like(GVF)
        load_gl[s].wait()

        def head(h, carry):
            pick = head_mask(h)
            for b, (lo, hi) in enumerate(windows):
                rows = slice(b * EDGE, (b + 1) * EDGE)
                cot = GC[rows, :] * pick
                grad_prob = dot_nt(cot, V[base + lo : base + hi, :])
                prob_low = PROB[s, h, rows, : hi - lo]
                prob = prob_low.astype(F32)
                term = prob * grad_prob
                level = jnp.sum(term, axis=-1, keepdims=True)
                grad = term - prob * level + GLB[s, h, rows, lo:hi].astype(F32)
                GLB[s, h, rows, lo:hi] = grad.astype(BF16)
                GVF[lo:hi, :] += dot_tn(prob_low, cot)
            grad_raw = GLB[s, h]
            GQF[...] += dot_nn(grad_raw, K[all_rows, :] * pick)
            GKF[...] += dot_tn(grad_raw, Q[all_rows, :] * pick)
            return carry

        lax.fori_loop(0, HEADS, head, 0)
        store = local(GLB.at[s], r_["glin_out"].at[s], 2 + s)
        for i, ref, scale in ((0, GQF, 0.125), (1, GKF, 0.125), (2, GVF, 1.0)):
            low = (ref[...] * scale).astype(BF16)
            GP[i, all_rows, :] = low
            if i != 1:
                row = 8 if i == 0 else 9
                SMG[row : row + 1, :C] += jnp.sum(low.astype(F32), axis=0, keepdims=True)

        def product(rows):
            total = dot_nt(GP[0, rows, :], WA[0])
            total = total + dot_nt(GP[1, rows, :], WA[1])
            return total + dot_nt(GP[2, rows, :], WA[2])

        return store, Reduction(2, s, product)

    def token_grads(s, total):
        total.wait()

        def body(r, carry):
            rows = token_rows(s, r)
            GT[rows, :] = (GS[s, pl.ds(r, TILE), :] + total.tile(r)).astype(BF16)
            return carry

        tile_loop(half, body, 0)
        return share(GT, s)

    class Scatter:
        def __init__(self, tag, fill):
            self.stage, self.yr = r_["ST" + tag], r_["YR" + tag]
            self.zs, self.zr = r_["ZS" + tag], r_["ZR" + tag]
            fill(self.stage)
            self.send_y = wires.send(self.stage.at[1 - y], self.yr, y_dev)

        def block(self, index):
            return self.stage[y, index].astype(F32) + self.yr[index].astype(F32)

        def along(self):
            self.send_y.wait_recv()
            self.sent = []
            for k in range(1, Z):
                self.zs[k - 1] = self.block(zto[k]).astype(BF16)
                self.sent.append(wires.send(self.zs.at[k - 1], self.zr.at[k - 1], z_dev[k]))

        def finish(self, out):
            total = self.block(z)
            for k in range(1, Z):
                self.sent[k - 1].wait_recv()
                total = total + self.zr[k - 1].astype(F32)
            out[...] = total

    def fill_square(left, right):
        def fill(stage):
            part = D // 2
            for i in range(2):
                product = dot_tn(left[:, i * part : (i + 1) * part], right[...]).astype(BF16)
                for j in range(part // SH):
                    index = i * (part // SH) + j
                    stage[index % Y, index // Y] = product[j * SH : (j + 1) * SH, :]

        return fill

    def fill_heads(stage):
        for a in range(4):
            left, right = (GAT, CTXF[...]) if a == 3 else (tok, GP[a])
            product = dot_tn(left[...], right).astype(BF16)
            for index in range(Z * Y):
                stage[index % Y, index // Y, a] = product[index * SH : (index + 1) * SH, :]

    store_l0, parts0 = attend(0)
    gather_u.forward()
    store_l1, parts1 = attend(1)
    gather_d.forward()
    wo_core.wait_recv()
    wo_x.wait_recv()
    wo_d = wires.send(WO.at[1], WO.at[2], c_dev)
    wo_d.wait_recv()
    normed0 = out_project(0, parts0)
    normed1 = out_project(1, parts1)
    gather_u.finish()
    normed0.wait_recv()
    feed_up(0)
    gather_d.finish()
    down0 = feed_down(0)
    normed1.wait_recv()
    feed_up(1)
    down0.cross()
    down1 = feed_down(1)
    down1.cross()
    branch0, mix0 = norm_two(0, down0)
    branch0.wait_recv()
    back0 = feed_back(0)
    back0.cross()
    branch1, mix1 = norm_two(1, down1)
    branch1.wait_recv()
    back1 = feed_back(1)
    back1.cross()
    scatter_d = Scatter("D", fill_square(BR, ACT))
    attn0 = norm_one_back(0, back0)
    attn0.wait_recv()
    store_g0, token0 = attend_back(0)
    token0.cross()
    scatter_d.along()
    scatter_u = Scatter("U", fill_square(NORMED, GH))
    attn1 = norm_one_back(1, back1)
    attn1.wait_recv()
    store_g1, token1 = attend_back(1)
    token1.cross()
    scatter_u.along()
    scatter_a = Scatter("A", fill_heads)
    small_core = wires.send(SMG, SMR.at[0], c_dev)
    mix0.wait_recv()
    mix1.wait_recv()
    store_mix = local(MIX, r_["mixed"], 4)
    share0 = token_grads(0, token0)
    small_core.wait_recv()
    upper = lax.broadcasted_iota(jnp.int32, SMG.shape, 0) < 8
    SMS[0] = SMG[...] + jnp.where(upper, SMR[0], 0.0)
    small_y = wires.send(SMS.at[0], SMR.at[1], y_dev)
    scatter_a.along()
    share1 = token_grads(1, token1)
    small_y.wait_recv()
    SMS[1] = SMS[0] + SMR[1]
    small_z = [wires.send(SMS.at[1], SMR.at[1 + k], z_dev[k]) for k in range(1, Z)]
    share0.wait_recv()
    share1.wait_recv()
    store_gt = local(GT, r_["gtok"], 5)
    scatter_d.finish(r_["gd"])
    scatter_u.finish(r_["gu"])
    scatter_a.finish(r_["ga"])
    small_total = SMS[1]
    for k in range(1, Z):
        small_z[k - 1].wait_recv()
        small_total = small_total + SMR[1 + k]
    r_["smg"][...] = small_total
    for copy in (store_l0, store_l1, store_g0, store_g1, store_mix, store_gt):
        copy.wait()
    wires.drain_all()


def fused_shards(
    tokens, segments, logits_in, w_qkv, w_out, w_up, w_down,
    head_bias, ff_bias, norm_gains, shift_biases, grad_out, grad_logits,
):
    rows, D = tokens.shape
    seqs, L = segments.shape
    HEADS = logits_in.shape[1]
    SH, unused, C = w_qkv.shape
    FF = w_up.shape[1]
    HD = C // HEADS
    half = L // 2
    width = max(D, FF)
    dpi = lax.axis_index("dp")

    def spread(array):
        piece = array.shape[1]
        wide = jnp.tile(array, (1, Z * Y))
        owner = lax.broadcasted_iota(jnp.int32, wide.shape, 1) // piece
        wide = jnp.where(owner == dpi, wide, 0)
        return jnp.pad(wide, ((0, 0), (0, width - wide.shape[1])))

    blank = jnp.zeros((2, width), BF16)
    small = jnp.concatenate(
        [
            spread(norm_gains),
            spread(shift_biases),
            blank,
            spread(head_bias),
            spread(ff_bias[None]),
            blank,
            blank,
            blank[:1],
        ],
        axis=0,
    )
    wa = jnp.stack([w_qkv[:, 0], w_qkv[:, 1], w_qkv[:, 2], w_out.T])
    dma = pltpu.SemaphoreType.DMA
    vm = pltpu.VMEM
    inputs = {
        "tok": tokens, "wa": wa, "wu": w_up, "wd": w_down.T, "sm": small, "seg": segments,
        "gout": grad_out, "lin": logits_in, "gl": grad_logits,
    }
    shape = jax.ShapeDtypeStruct
    outputs = {
        "mixed": shape((rows, D), BF16),
        "logits_out": shape(logits_in.shape, BF16),
        "gtok": shape((rows, D), BF16),
        "glin_out": shape(logits_in.shape, BF16),
        "ga": shape((4, SH, C), F32),
        "gu": shape((SH, FF), F32),
        "gd": shape((SH, FF), F32),
        "smg": shape((16, width), F32),
    }
    scratch = {
        "WA": vm((4, D, C), BF16), "WU": vm((D, FF), BF16), "WD": vm((D, FF), BF16),
        "SM": vm((Z * Y, 16, width), BF16), "SMV": vm((16, width), F32), "WO": vm((3, D, C), BF16),
        "GOUT": vm((seqs, half, D), BF16),
        "Q": vm((rows, C), BF16), "K": vm((rows, C), BF16), "V": vm((rows, C), BF16),
        "LIN": vm(logits_in.shape, BF16), "GLB": vm(logits_in.shape, BF16),
        "PROB": vm((seqs, HEADS, L, 3 * EDGE), BF16), "BIAS": vm((L, 3 * EDGE), F32),
        "CTXF": vm((rows, C), BF16), "CTXR": vm((3, seqs, half, C), BF16),
        "NORMED": vm((rows, D), BF16), "ACT": vm((rows, FF), BF16), "DG": vm((rows, FF), F32),
        "BR": vm((rows, D), BF16), "GH": vm((rows, FF), BF16), "GAT": vm((rows, D), BF16),
        "GC": vm((L, C), BF16), "MIX": vm((rows, D), BF16), "GT": vm((rows, D), BF16),
        "XH1": vm((seqs, half, D), F32), "R1": vm((seqs, half, EDGE), F32),
        "GS": vm((seqs, half, D), F32), "HB": vm((CHUNK, width), F32),
        "OWN": vm((seqs, half, D), F32), "CS": vm((seqs, half, D), BF16),
        "CR": vm((seqs, half, D), BF16), "XS": vm((seqs, half, D), BF16),
        "XR": vm((3, seqs, half, D), BF16), "GP": vm((3, rows, C), BF16),
        "GQF": vm((L, C), F32), "GKF": vm((L, C), F32), "GVF": vm((L, C), F32),
        "SMG": vm((16, width), F32), "SMS": vm((2, 16, width), F32), "SMR": vm((5, 16, width), F32),
        "send_sem": dma((COPIES,)), "recv_sem": dma((COPIES,)), "local_sem": dma((8,)),
    }
    for tag, block in (("A", (4, SH, C)), ("U", (SH, FF)), ("D", (SH, FF))):
        scratch["ST" + tag] = vm((Y, Z) + block, BF16)
        scratch["YR" + tag] = vm((Z,) + block, BF16)
        scratch["ZS" + tag] = vm((Z - 1,) + block, BF16)
        scratch["ZR" + tag] = vm((Z - 1,) + block, BF16)
    near, far = pl.BlockSpec(memory_space=pltpu.VMEM), pl.BlockSpec(memory_space=pl.ANY)
    distant = ("gout", "lin", "gl", "mixed", "logits_out", "gtok", "glin_out")
    names = (*inputs, *outputs, *scratch)
    dims = (L, HEADS, HD, D, FF, C, SH)
    results = pl.pallas_call(
        functools.partial(layer_kernel, names, dims),
        out_shape=tuple(outputs.values()),
        in_specs=[far if name in distant else near for name in inputs],
        out_specs=tuple(far if name in distant else near for name in outputs),
        scratch_shapes=list(scratch.values()),
        compiler_params=pltpu.CompilerParams(
            collective_id=0, has_side_effects=True, vmem_limit_bytes=66 * 1000 * 1000
        ),
    )(*inputs.values())
    mixed, logits_out, gtok, glin, ga, gu, gd, smg = results

    def own(first, last, piece):
        return lax.dynamic_slice(smg, (first, dpi * piece), (last - first, piece))

    return (
        mixed,
        logits_out,
        gtok,
        glin,
        jnp.transpose(ga[:3], (1, 0, 2)),
        ga[3].T,
        gu,
        gd.T,
        own(8, 10, head_bias.shape[1]),
        own(10, 11, ff_bias.shape[0])[0],
        own(0, 2, SH),
        own(2, 6, SH),
    )


def solution(mesh):
    body = fused_shards if mesh.shape["dp"] == Z * Y and mesh.shape["mp"] == 4 else shards
    return jax.shard_map(
        body,
        mesh=mesh,
        in_specs=(
            P("dp", None),
            P("dp", None),
            P("dp", "mp", None, None),
            P("dp", None, "mp"),
            P("mp", "dp"),
            P("dp", "mp"),
            P("mp", "dp"),
            P(None, ("mp", "dp")),
            P(("mp", "dp")),
            P(None, "dp"),
            P(None, "dp"),
            P("dp", None),
            P("dp", "mp", None, None),
        ),
        out_specs=(
            P("dp", None),
            P("dp", "mp", None, None),
            P("dp", None),
            P("dp", "mp", None, None),
            P("dp", None, "mp"),
            P("mp", "dp"),
            P("dp", "mp"),
            P("mp", "dp"),
            P(None, ("mp", "dp")),
            P(("mp", "dp")),
            P(None, "dp"),
            P(None, "dp"),
        ),
        check_vma=False,
    )
```

```python
import functools

import jax
import jax.numpy as jnp
from jax import lax
from jax.experimental import pallas as pl
from jax.experimental.pallas import tpu as pltpu
from jax.sharding import PartitionSpec as P

MB = 2
MESH = pl.DeviceIdType.MESH
F32 = jnp.float32
BF16 = jnp.bfloat16

epsilon = 1e-05
masked_value = -10000.0


def norm_rows(hidden, gain, shift):
    center = hidden - jnp.mean(hidden, axis=-1, keepdims=True)
    spread = jnp.mean(center * center, axis=-1, keepdims=True)
    return center * lax.rsqrt(spread + epsilon) * gain + shift


def gelu_exact(value):
    return 0.5 * value * (1.0 + lax.erf(value * 0.7071067811865476))


def add_trees(first_tree, second_tree):
    if first_tree is None:
        return second_tree
    return jax.tree.map(jnp.add, first_tree, second_tree)


def micro_step(whole, block_tokens, block_segments, block_logits, block_grad, block_grad_logits):
    qkv_weight, out_weight, up_weight, down_weight, bias_heads, bias_hidden, gains, shifts = whole
    seq_count = block_segments.shape[0]
    length = block_segments.shape[1]
    feature = block_tokens.shape[1]
    row_count = block_tokens.shape[0]
    local_heads = block_logits.shape[1]
    flat_qkv = qkv_weight.reshape(feature, -1)
    local_cols = flat_qkv.shape[1] // 3
    head_size = local_cols // local_heads
    gain_rows = gains.astype(jnp.float32)
    shift_rows = shifts.astype(jnp.float32)
    head_rows = bias_heads.astype(jnp.float32)
    shape_heads = (seq_count, length, local_heads, head_size)
    token_float = block_tokens.astype(jnp.float32)
    projected = jnp.dot(block_tokens, flat_qkv, preferred_element_type=jnp.float32)
    query = (projected[:, :local_cols] + head_rows[0]).astype(jnp.bfloat16).reshape(shape_heads)
    keys = projected[:, local_cols : 2 * local_cols].astype(jnp.bfloat16).reshape(shape_heads)
    values = (
        (projected[:, 2 * local_cols :] + head_rows[1]).astype(jnp.bfloat16).reshape(shape_heads)
    )
    same = block_segments[:, :, None] == block_segments[:, None, :]
    mask = jnp.where(same, 0.0, masked_value).astype(jnp.float32)[:, None]
    incoming = block_logits.astype(jnp.float32)
    raw = (
        jnp.einsum("sqhd,skhd->shqk", query, keys, preferred_element_type=jnp.float32) * 0.125
        + incoming
    )
    shifted = raw + mask
    top = jnp.max(shifted, axis=-1, keepdims=True)
    expo = jnp.exp(shifted - top)
    total = jnp.sum(expo, axis=-1, keepdims=True)
    log_total = top + jnp.log(total)
    context = jnp.einsum(
        "shqk,skhd->sqhd",
        (expo / total).astype(jnp.bfloat16),
        values,
        preferred_element_type=jnp.float32,
    )
    context = context.reshape(row_count, local_cols).astype(jnp.bfloat16)
    attn_total = lax.psum(jnp.dot(context, out_weight, preferred_element_type=jnp.float32), "mp")
    first_pre = attn_total + shift_rows[0] + token_float
    normed = norm_rows(first_pre, gain_rows[0], shift_rows[1]).astype(jnp.bfloat16)
    hidden_pre = jnp.dot(
        normed, up_weight, preferred_element_type=jnp.float32
    ) + bias_hidden.astype(jnp.float32)
    activated = gelu_exact(hidden_pre).astype(jnp.bfloat16)
    ffn_total = lax.psum(jnp.dot(activated, down_weight, preferred_element_type=jnp.float32), "mp")
    second_pre = ffn_total + shift_rows[2] + normed.astype(jnp.float32)
    cotangent = block_grad.astype(jnp.float32)
    mixed_part = norm_rows(second_pre, gain_rows[1], shift_rows[3]).astype(jnp.bfloat16)
    unused_second, second_pull = jax.vjp(norm_rows, second_pre, gain_rows[1], shift_rows[3])
    grad_second, grad_gain_two, grad_shift_two = second_pull(cotangent)
    branch_part = grad_second.astype(jnp.bfloat16)
    grad_bias_two = jnp.sum(branch_part.astype(jnp.float32), axis=0)
    grad_down = jnp.einsum("rf,rd->fd", activated, branch_part, preferred_element_type=jnp.float32)
    grad_act = jnp.einsum("rd,fd->rf", branch_part, down_weight, preferred_element_type=jnp.float32)
    unused_gelu, gelu_pull = jax.vjp(gelu_exact, hidden_pre)
    grad_hidden = gelu_pull(grad_act)[0].astype(jnp.bfloat16)
    grad_bias_hidden = jnp.sum(grad_hidden.astype(jnp.float32), axis=0)
    grad_up = jnp.einsum("rd,rf->df", normed, grad_hidden, preferred_element_type=jnp.float32)
    hidden_terms = jnp.einsum(
        "rf,df->rd", grad_hidden, up_weight, preferred_element_type=jnp.float32
    )
    grad_normed = grad_second + lax.psum(hidden_terms, "mp")
    unused_first, first_pull = jax.vjp(norm_rows, first_pre, gain_rows[0], shift_rows[1])
    grad_first, grad_gain_one, grad_shift_one = first_pull(grad_normed)
    grad_attn = grad_first.astype(jnp.bfloat16)
    grad_bias_out = jnp.sum(grad_attn.astype(jnp.float32), axis=0)
    grad_out_weight = jnp.einsum(
        "rc,rd->cd", context, grad_attn, preferred_element_type=jnp.float32
    )
    grad_context = jnp.einsum(
        "rd,cd->rc", grad_attn, out_weight, preferred_element_type=jnp.float32
    )
    grad_context = grad_context.astype(jnp.bfloat16).reshape(shape_heads)
    raw_again = (
        jnp.einsum("sqhd,skhd->shqk", query, keys, preferred_element_type=jnp.float32) * 0.125
        + incoming
    )
    prob = jnp.exp(raw_again + mask - log_total)
    grad_prob = jnp.einsum(
        "sqhd,skhd->shqk", grad_context, values, preferred_element_type=jnp.float32
    )
    grad_raw = prob * (
        grad_prob - jnp.sum(prob * grad_prob, axis=-1, keepdims=True)
    ) + block_grad_logits.astype(jnp.float32)
    grad_raw_low = grad_raw.astype(jnp.bfloat16)
    grad_query = (
        jnp.einsum("shqk,skhd->sqhd", grad_raw_low, keys, preferred_element_type=jnp.float32)
        * 0.125
    )
    grad_keys = (
        jnp.einsum("shqk,sqhd->skhd", grad_raw_low, query, preferred_element_type=jnp.float32)
        * 0.125
    )
    grad_values = jnp.einsum(
        "shqk,sqhd->skhd",
        prob.astype(jnp.bfloat16),
        grad_context,
        preferred_element_type=jnp.float32,
    )
    grad_query = grad_query.astype(jnp.bfloat16).reshape(row_count, local_cols)
    grad_keys = grad_keys.astype(jnp.bfloat16).reshape(row_count, local_cols)
    grad_values = grad_values.astype(jnp.bfloat16).reshape(row_count, local_cols)
    grad_proj = jnp.concatenate([grad_query, grad_keys, grad_values], axis=1)
    grad_qkv = jnp.einsum(
        "rd,rc->dc", block_tokens, grad_proj, preferred_element_type=jnp.float32
    ).reshape(qkv_weight.shape)
    grad_heads = jnp.stack(
        [
            jnp.sum(grad_query.astype(jnp.float32), axis=0),
            jnp.sum(grad_values.astype(jnp.float32), axis=0),
        ]
    )
    input_terms = jnp.einsum("rc,dc->rd", grad_proj, flat_qkv, preferred_element_type=jnp.float32)
    grad_inputs = grad_first + lax.psum(input_terms.astype(jnp.bfloat16), "mp").astype(jnp.float32)
    results = (mixed_part, raw.astype(jnp.bfloat16), grad_inputs.astype(jnp.bfloat16), grad_raw_low)
    grads = (
        grad_qkv,
        grad_out_weight,
        grad_up,
        grad_down,
        grad_heads,
        grad_bias_hidden,
        jnp.stack([grad_gain_one, grad_gain_two]),
        jnp.stack([grad_bias_out, grad_shift_one, grad_bias_two, grad_shift_two]),
    )
    return (results, grads)


def shards(
    tokens,
    segments,
    logits_in,
    w_qkv,
    w_out,
    w_up,
    w_down,
    head_bias,
    ff_bias,
    norm_gains,
    shift_biases,
    grad_out,
    grad_logits,
):
    seq_count = segments.shape[0] // MB
    row_count = seq_count * segments.shape[1]
    collected = []
    totals = None
    for micro in range(MB):
        whole = (
            lax.all_gather(w_qkv, "dp", axis=0, tiled=True),
            lax.all_gather(w_out, "dp", axis=1, tiled=True),
            lax.all_gather(w_up, "dp", axis=0, tiled=True),
            lax.all_gather(w_down, "dp", axis=1, tiled=True),
            lax.all_gather(head_bias, "dp", axis=1, tiled=True),
            lax.all_gather(ff_bias, "dp", axis=0, tiled=True),
            lax.all_gather(norm_gains, "dp", axis=1, tiled=True),
            lax.all_gather(shift_biases, "dp", axis=1, tiled=True),
        )
        first_row = micro * row_count
        first_seq = micro * seq_count
        results, grads = micro_step(
            whole,
            tokens[first_row : first_row + row_count],
            segments[first_seq : first_seq + seq_count],
            logits_in[first_seq : first_seq + seq_count],
            grad_out[first_row : first_row + row_count],
            grad_logits[first_seq : first_seq + seq_count],
        )
        totals = add_trees(totals, grads)
        collected.append(results)
    totals = (
        lax.psum_scatter(totals[0], "dp", scatter_dimension=0, tiled=True),
        lax.psum_scatter(totals[1], "dp", scatter_dimension=1, tiled=True),
        lax.psum_scatter(totals[2], "dp", scatter_dimension=0, tiled=True),
        lax.psum_scatter(totals[3], "dp", scatter_dimension=1, tiled=True),
        lax.psum_scatter(totals[4], "dp", scatter_dimension=1, tiled=True),
        lax.psum_scatter(totals[5], "dp", scatter_dimension=0, tiled=True),
        lax.psum_scatter(totals[6], "dp", scatter_dimension=1, tiled=True),
        lax.psum_scatter(totals[7], "dp", scatter_dimension=1, tiled=True),
    )
    mixed = jnp.concatenate([item[0] for item in collected], axis=0)
    logits_out = jnp.concatenate([item[1] for item in collected], axis=0)
    grad_tokens = jnp.concatenate([item[2] for item in collected], axis=0)
    grad_logits_in = jnp.concatenate([item[3] for item in collected], axis=0)
    return (
        mixed,
        logits_out,
        grad_tokens,
        grad_logits_in,
        totals[0],
        totals[1],
        totals[2],
        totals[3],
        totals[4],
        totals[5],
        totals[6],
        totals[7],
    )


Z, Y, CORES = 4, 2, 2
TILE = 32
EDGE = 128
CHUNK = 256
COPIES = 144


def dot_nn(a, b):
    return lax.dot_general(a, b, (((1,), (0,)), ((), ())), preferred_element_type=F32)


def dot_nt(a, b):
    return lax.dot_general(a, b, (((1,), (1,)), ((), ())), preferred_element_type=F32)


def dot_tn(a, b):
    return lax.dot_general(a, b, (((0,), (0,)), ((), ())), preferred_element_type=F32)


def fold_rows(value):
    rows, cols = value.shape
    return jnp.sum(value.reshape(rows // 8, 8, cols), axis=0)


class Wires:
    def __init__(self, send_sem, recv_sem):
        self.send_sem, self.recv_sem, self.sent, self.drained = send_sem, recv_sem, [], []
        self.slots = 0

    def take(self, count):
        self.slots += count
        return self.slots - count

    def describe(self, src, dst, device, out, into):
        return pltpu.make_async_remote_copy(
            src_ref=src,
            dst_ref=dst,
            send_sem=self.send_sem.at[out],
            recv_sem=self.recv_sem.at[into],
            device_id=device,
            device_id_type=MESH,
        )

    def send(self, src, dst, device, into=None):
        copy = self.describe(
            src, dst, device, len(self.sent), self.take(1) if into is None else into
        )
        copy.start()
        self.sent.append(copy)
        return copy

    def send_if(self, condition, src, dst, device, into):
        copy = self.describe(src, dst, device, len(self.sent), into)
        pl.when(condition)(copy.start)
        self.sent.append((copy, condition))

    def arrived(self, ref, device, into):
        self.describe(ref, ref, device, 0, into).wait_recv()

    def drain(self, copy):
        copy.wait_send()
        self.drained.append(copy)

    def drain_all(self):
        for copy in self.sent:
            if isinstance(copy, tuple):
                pl.when(copy[1])(copy[0].wait_send)
            elif not any(copy is done for done in self.drained):
                copy.wait_send()


def layer_kernel(names, dims, *refs):
    r_ = dict(zip(names, refs, strict=True))
    L, HEADS, HD, D, FF, C, SH = dims
    seqs = 2
    half = L // 2
    tok, seg, GOUT = r_["tok"], r_["seg"], r_["GOUT"]
    WA, WU, WD, WO, SMV = r_["WA"], r_["WU"], r_["WD"], r_["WO"], r_["SMV"]
    Q, K, V, LIN, GLB, PROB = r_["Q"], r_["K"], r_["V"], r_["LIN"], r_["GLB"], r_["PROB"]
    BIAS, CTXF, CTXR = r_["BIAS"], r_["CTXF"], r_["CTXR"]
    NORMED, ACT, DG, BR, GH, GAT = r_["NORMED"], r_["ACT"], r_["DG"], r_["BR"], r_["GH"], r_["GAT"]
    GC, MIX, GT, XH1, R1, GS = r_["GC"], r_["MIX"], r_["GT"], r_["XH1"], r_["R1"], r_["GS"]
    HB, CS, CR, XS, XR = r_["HB"], r_["CS"], r_["CR"], r_["XS"], r_["XR"]
    OWN, GP = r_["OWN"], r_["GP"]
    GQF, GKF, GVF = r_["GQF"], r_["GKF"], r_["GVF"]
    SMG, SMS, SMR = r_["SMG"], r_["SMS"], r_["SMR"]
    local_sem = r_["local_sem"]

    dpi, mpi = lax.axis_index("dp"), lax.axis_index("mp")
    z, y = lax.div(dpi, Y), lax.rem(dpi, Y)
    x, core = lax.div(mpi, CORES), lax.rem(mpi, CORES)
    wires = Wires(r_["send_sem"], r_["recv_sem"])

    def dev(zz, yy, xx, cc):
        return {"dp": zz * Y + yy, "mp": xx * CORES + cc}

    zto = [lax.rem(z + k, Z) for k in range(Z)]
    zfrom = [lax.rem(z - k + Z, Z) for k in range(Z)]
    z_dev = [dev(zto[k], y, x, core) for k in range(Z)]
    y_dev = dev(z, 1 - y, x, core)
    c_dev = dev(z, y, x, 1 - core)
    x_dev = dev(z, y, 1 - x, core)
    d_dev = dev(z, y, 1 - x, 1 - core)

    def local(src, dst, index):
        copy = pltpu.make_async_copy(src, dst, local_sem.at[index])
        copy.start()
        return copy

    load_lin = [local(r_["lin"].at[s], LIN.at[s], s) for s in range(seqs)]
    load_tok = local(r_["tok_far"], tok, 6)
    load_gout = [
        local(r_["gout"].at[pl.ds(pl.multiple_of(s * L + core * half, half), half), :], GOUT.at[s], 4 + s)
        for s in range(seqs)
    ]
    load_gl = [local(r_["gl"].at[s], GLB.at[s], 2 + s) for s in range(seqs)]

    def iotas(rows, cols):
        down = lax.broadcasted_iota(jnp.int32, (rows, cols), 0)
        return down, lax.broadcasted_iota(jnp.int32, (rows, cols), 1)

    def shifted(rows, cols, by):
        down, over = iotas(rows, cols)
        return jnp.where(over - down == by, 1.0, 0.0).astype(BF16)

    PAIR = 2 * EDGE
    PK, wa = r_["PK"], r_["wa"]
    even, odd = shifted(C, PAIR, 0), shifted(C, PAIR, PAIR - C)
    out_low = dot_nt(shifted(SH, SH, 0), r_["wo"][...]).astype(BF16)
    for at, first, second in ((0, wa[0], wa[2]), (3 * EDGE, wa[1], out_low)):
        first, second = dot_nn(first, even), dot_nn(second, odd)
        PK[:, at : at + EDGE] = first[:, :EDGE].astype(BF16)
        PK[:, at + EDGE : at + PAIR] = (first[:, EDGE:] + second[:, :EDGE]).astype(BF16)
        PK[:, at + PAIR : at + 3 * EDGE] = second[:, EDGE:].astype(BF16)

    barrier = pltpu.get_barrier_semaphore()
    friends = z_dev[1:] + [y_dev, c_dev, x_dev, d_dev]
    for friend in friends:
        pl.semaphore_signal(barrier, inc=1, device_id=friend, device_id_type=MESH)
    pl.semaphore_wait(barrier, len(friends))

    near = z - 1 + 2 * lax.div(3 - z, 3)
    last = 3 * (1 - lax.div(z, 2))
    order = [near, 6 - z - near - last, last]

    class Gather:
        def __init__(self, src, dst, place):
            self.src, self.dst, self.place = src, dst, place
            self.z_in, self.y_in = wires.take(Z), wires.take(Z)

        def along(self):
            here = self.dst.at[self.place(dpi)]
            for there in order:
                wires.send(self.src, here, dev(there, y, x, core), self.z_in + z)

        def across(self):
            wires.send(self.src, self.dst.at[self.place(dpi)], y_dev, self.y_in + z)

        def keep(self):
            self.dst[self.place(dpi)] = self.src[...]

        def forward(self, step):
            origin = order[step]
            block = self.dst.at[self.place(origin * Y + y)]
            wires.arrived(block, y_dev, self.z_in + origin)
            wires.send(block, block, y_dev, self.y_in + origin)

        def finish(self):
            for origin in range(Z):
                block = self.dst.at[self.place(origin * Y + 1 - y)]
                wires.arrived(block, y_dev, self.y_in + origin)

    class Line(Gather):
        def push(self, src, origin, held):
            block = self.dst.at[self.place(origin * Y + y)]
            if src is None:
                src = block
            ways = ((z < Z - 1, jnp.minimum(z + 1, Z - 1), 0), (z > 0, jnp.maximum(z - 1, 0), 1))
            for room, there, side in ways:
                if held is None or held[1] == side:
                    going = room if held is None else jnp.logical_and(room, held[0])
                    wires.send_if(going, src, block, dev(there, y, x, core), self.z_in + origin)
            if held is None:
                wires.send(src, block, y_dev, self.y_in + origin)
            else:
                wires.send_if(held[0], src, block, y_dev, self.y_in + origin)

        def start(self):
            self.push(self.src, z, None)

        def step(self, hop):
            for side, origin, held in ((0, z - hop, z >= hop), (1, z + hop, z + hop < Z)):
                block = self.dst.at[self.place(jnp.clip(origin, 0, Z - 1) * Y + y)]

                @pl.when(held)
                def arrive():
                    wires.arrived(block, y_dev, self.z_in + origin)

                self.push(None, jnp.clip(origin, 0, Z - 1), (held, side))

    def rows_of(index):
        return pl.ds(pl.multiple_of(index * SH, SH), SH)

    def by_rows(index):
        return (rows_of(index), slice(None))

    def by_lanes(index):
        return (slice(None), pl.ds(pl.multiple_of(index * EDGE, EDGE), EDGE))

    SMB, SM = r_["SMB"], r_["SM"]
    gather_a = Line(PK, WA, by_rows)
    gather_s = Gather(SMB, SM, by_lanes)
    gather_u = Gather(r_["wu"], WU, by_rows)
    gather_d = Gather(r_["wd"], WD, by_rows)

    gather_a.start()

    blend = r_["BLEND"]
    blend[...] = jnp.zeros_like(blend)
    blend[0:2, :SH] = r_["gains"][...].astype(F32)
    blend[2:6, :SH] = r_["shifts"][...].astype(F32)
    piece = r_["hbias"].shape[1]
    blend[8:10, :piece] = r_["hbias"][...].astype(F32)
    blend[10:11, :SH] = r_["fbias"][...].astype(F32)
    SMB[...] = blend[...].astype(BF16)
    gather_s.along()
    gather_s.across()

    for gather in (gather_a, gather_s, gather_u, gather_d):
        gather.keep()
    load_tok.wait()
    gather_a.step(1)
    for i in range(Z * Y):
        rows = slice(i * EDGE, (i + 1) * EDGE)
        down, over = iotas(EDGE, GH.shape[1])
        GH[rows, :] = jnp.where((over - down == i * SH) & (down < SH), 1.0, 0.0).astype(BF16)
        down, over = iotas(EDGE, 2 * PAIR)
        gap = i * piece + jnp.where(over < PAIR, 0, PAIR + PAIR - C)
        ACT[rows, : 2 * PAIR] = jnp.where(
            (over - down == gap) & (down < piece), 1.0, 0.0
        ).astype(BF16)

    gather_a.step(2)
    gather_a.step(3)
    for step in range(Z - 1):
        gather_s.forward(step)
    gather_a.finish()
    gather_s.finish()
    gather_u.along()
    gather_d.along()
    gather_u.across()
    gather_d.across()
    outer = WA.at[:, 4 * EDGE : 6 * EDGE]
    wo_core = wires.send(outer, WO.at[0], c_dev)
    wo_x = wires.send(outer, WO.at[1], x_dev)

    SMV[...] = dot_nn(SM[...], GH[...])
    r_["HBV"][...] = dot_nn(SM[...], ACT[:, : 2 * PAIR])
    SMG[...] = jnp.zeros_like(SMG)

    def vec(row, width=D):
        return SMV[row : row + 1, :width]

    def project(i, carry):
        rows = pl.ds(pl.multiple_of(i * CHUNK, CHUNK), CHUNK)
        block = tok[rows, :]
        HBV = r_["HBV"]
        Q[rows, :] = (dot_nn(block, WA[:, :PAIR]) + HBV[8:9, :PAIR]).astype(BF16)
        V[rows, :] = (dot_nn(block, WA[:, EDGE : 3 * EDGE]) + HBV[9:10, PAIR:]).astype(BF16)
        K[rows, :] = dot_nn(block, WA[:, 3 * EDGE : 5 * EDGE]).astype(BF16)
        return carry

    lax.fori_loop(0, seqs * L // CHUNK, project, 0)

    lanes = lax.broadcasted_iota(jnp.int32, (1, PAIR), 1)

    def head_mask(h, start=0):
        inside = (lanes >= start + h * HD) & (lanes < start + (h + 1) * HD)
        return jnp.where(inside, 1.0, 0.0).astype(BF16)

    blocks = L // EDGE
    windows = [(max(b - 1, 0) * EDGE, min(b + 2, blocks) * EDGE) for b in range(blocks)]

    def half_of(s, which):
        return pl.ds(pl.multiple_of(s * L + which * half, half), half)

    def mine(s):
        return half_of(s, core)

    def theirs(s):
        return half_of(s, 1 - core)

    def attend(s, between):
        base = s * L
        ids = seg[s : s + 1, :].astype(F32)
        tall = jnp.transpose(jnp.broadcast_to(ids, (EDGE, L)))
        for b, (lo, hi) in enumerate(windows):
            for j in range((hi - lo) // EDGE):
                near = ids[:, lo + j * EDGE : lo + (j + 1) * EDGE]
                same = tall[b * EDGE : (b + 1) * EDGE, :] == near
                BIAS[b * EDGE : (b + 1) * EDGE, j * EDGE : (j + 1) * EDGE] = jnp.where(
                    same, 0.0, masked_value
                ).astype(F32)
        GQF[...] = jnp.zeros_like(GQF)
        load_lin[s].wait()

        for h in range(HEADS):
            pick, pick_v = head_mask(h), head_mask(h, PAIR - C)
            for b, (lo, hi) in enumerate(windows):
                rows = slice(b * EDGE, (b + 1) * EDGE)
                query = Q[base + b * EDGE : base + (b + 1) * EDGE, :] * pick
                score = dot_nt(query, K[base : base + L, :])
                raw = score * 0.125 + LIN[s, h, rows, :].astype(F32)
                LIN[s, h, rows, :] = raw.astype(BF16)
                near = raw[:, lo:hi] + BIAS[rows, : hi - lo]
                top = jnp.max(near, axis=-1, keepdims=True)
                expo = jnp.exp(near - top)
                norm = 1.0 / jnp.sum(expo, axis=-1, keepdims=True)
                prob = (expo * norm).astype(BF16)
                PROB[s, h, rows, : hi - lo] = prob
                GQF[rows, :] += dot_nn(prob, V[base + lo : base + hi, :] * pick_v)
            for job in between[h]:
                job()
        CTXF[base : base + L, :] = GQF[...].astype(BF16)
        store = local(LIN.at[s], r_["logits_out"].at[s], s)
        parts = [
            wires.send(CTXF.at[theirs(s), :], CTXR.at[0, s], c_dev),
            wires.send(CTXF.at[mine(s), :], CTXR.at[1, s], x_dev),
            wires.send(CTXF.at[theirs(s), :], CTXR.at[2, s], d_dev),
        ]
        return store, parts

    def tile_loop(count, body, init):
        def step(i, carry):
            return body(pl.multiple_of(i * TILE, TILE), carry)

        return lax.fori_loop(0, count // TILE, step, init)

    def token_rows(s, r):
        return pl.ds(pl.multiple_of(s * L + core * half + r, TILE), TILE)

    def normalize(value):
        center = value - jnp.mean(value, axis=-1, keepdims=True)
        spread = jnp.mean(center * center, axis=-1, keepdims=True)
        scale = lax.rsqrt(spread + epsilon)
        return center * scale, scale

    def norm_back(scaled, xhat, scale):
        flat = jnp.mean(scaled, axis=-1, keepdims=True)
        tilt = jnp.mean(scaled * xhat, axis=-1, keepdims=True)
        return scale * (scaled - flat - xhat * tilt)

    def add_small(rows, sums):
        for row, value in zip(rows, sums, strict=True):
            SMG[row : row + 1, :] += jnp.sum(value, axis=0, keepdims=True)

    def share(ref, s):
        return wires.send(ref.at[mine(s), :], ref.at[mine(s), :], c_dev)

    def out_project(s, parts):
        for copy in parts:
            copy.wait_recv()
        HB[...] = dot_nt(CTXF[mine(s), :], outer[...]) + dot_nt(CTXR[0, s], WO[0])
        OWN[s] = dot_nt(CTXR[1, s], WO[1]) + dot_nt(CTXR[2, s], WO[2])

        def body(r, carry):
            at = pl.ds(r, TILE)
            first = (HB[at, :] + OWN[s, at, :]) + vec(2) + tok[token_rows(s, r), :].astype(F32)
            xhat, scale = normalize(first)
            XH1[s, at, :] = xhat
            R1[s, at, :] = jnp.broadcast_to(scale, (TILE, EDGE))
            NORMED[token_rows(s, r), :] = (xhat * vec(0) + vec(3)).astype(BF16)
            return carry

        tile_loop(half, body, 0)
        return share(NORMED, s)

    def feed_up(s):
        def block(i, carry):
            start = s * L + i * CHUNK
            rows = pl.ds(pl.multiple_of(start, CHUNK), CHUNK)
            HB[...] = dot_nn(NORMED[rows, :], WU[...]) + vec(10, FF)

            def body(r, inner):
                to = pl.ds(pl.multiple_of(start + r, TILE), TILE)
                value = HB[pl.ds(r, TILE), :]
                cdf = 0.5 * (1.0 + lax.erf(value * 0.7071067811865476))
                ACT[to, :] = (value * cdf).astype(BF16)
                DG[to, :] = cdf + value * (jnp.exp(-0.5 * value * value) * 0.3989422804014327)
                return inner

            return tile_loop(CHUNK, body, carry)

        lax.fori_loop(0, L // CHUNK, block, 0)

    last_sum = [None] * seqs

    class Reduction:
        def __init__(self, stage, s, product):
            self.stage, self.s = stage, s
            before = last_sum[s]
            if before is not None:
                wires.drain(before.pair)
                wires.drain(before.far)
            last_sum[s] = self
            CS[s] = product(theirs(s)).astype(BF16)
            self.pair = wires.send(CS.at[s], CR.at[s], c_dev)
            OWN[s] = product(mine(s))

        def cross(self):
            s = self.s
            self.pair.wait_recv()
            XS[s] = (OWN[s] + CR[s].astype(F32)).astype(BF16)
            self.far = wires.send(XS.at[s], XR.at[self.stage, s], x_dev)

        def wait(self):
            self.far.wait_recv()

        def tile(self, r):
            at = pl.ds(r, TILE)
            return XS[self.s, at, :].astype(F32) + XR[self.stage, self.s, at, :].astype(F32)

    def feed_down(s):
        return Reduction(0, s, lambda rows: dot_nt(ACT[rows, :], WD[...]))

    zeros = jnp.zeros((8, D), F32)

    def norm_two(s, total):
        load_gout[s].wait()

        def body(r, carry):
            gain, shift, bias = carry
            rows = token_rows(s, r)
            second = total.tile(r) + vec(4) + NORMED[rows, :].astype(F32)
            xhat, scale = normalize(second)
            MIX[rows, :] = (xhat * vec(1) + vec(5)).astype(BF16)
            cot = GOUT[s, pl.ds(r, TILE), :].astype(F32)
            back = norm_back(cot * vec(1), xhat, scale)
            GS[s, pl.ds(r, TILE), :] = back
            low = back.astype(BF16)
            BR[rows, :] = low
            gain = gain + fold_rows(cot * xhat)
            shift = shift + fold_rows(cot)
            bias = bias + fold_rows(low.astype(F32))
            return gain, shift, bias

        add_small((1, 5, 4), tile_loop(half, body, (zeros, zeros, zeros)))
        return share(BR, s), share(MIX, s)

    def feed_back(s):
        def block(i, carry):
            start = s * L + i * CHUNK
            rows = pl.ds(pl.multiple_of(start, CHUNK), CHUNK)
            HB[...] = dot_nn(BR[rows, :], WD[...])

            def body(r, total):
                to = pl.ds(pl.multiple_of(start + r, TILE), TILE)
                low = (HB[pl.ds(r, TILE), :] * DG[to, :]).astype(BF16)
                GH[to, :] = low
                return total + fold_rows(low.astype(F32))

            return tile_loop(CHUNK, body, carry)

        sums = lax.fori_loop(0, L // CHUNK, block, jnp.zeros((8, FF), F32))
        SMG[10:11, :FF] += jnp.sum(sums, axis=0, keepdims=True)
        return Reduction(1, s, lambda rows: dot_nt(GH[rows, :], WU[...]))

    def norm_one_back(s, total):
        def body(r, carry):
            gain, shift, bias = carry
            at = pl.ds(r, TILE)
            cot = GS[s, at, :] + total.tile(r)
            xhat = XH1[s, at, :]
            back = norm_back(cot * vec(0), xhat, R1[s, at, 0:1])
            GS[s, at, :] = back
            low = back.astype(BF16)
            GAT[token_rows(s, r), :] = low
            gain = gain + fold_rows(cot * xhat)
            shift = shift + fold_rows(cot)
            bias = bias + fold_rows(low.astype(F32))
            return gain, shift, bias

        add_small((0, 3, 2), tile_loop(half, body, (zeros, zeros, zeros)))
        return share(GAT, s)

    def attend_back(s, between):
        base = s * L
        all_rows = slice(base, base + L)
        GC[...] = dot_nn(GAT[all_rows, :], outer[...]).astype(BF16)
        GQF[...] = jnp.zeros_like(GQF)
        GKF[...] = jnp.zeros_like(GKF)
        GVF[...] = jnp.zeros_like(GVF)
        load_gl[s].wait()

        for h in range(HEADS):
            pick, pick_v = head_mask(h), head_mask(h, PAIR - C)
            for b, (lo, hi) in enumerate(windows):
                rows = slice(b * EDGE, (b + 1) * EDGE)
                cot = GC[rows, :] * pick_v
                grad_prob = dot_nt(cot, V[base + lo : base + hi, :])
                prob_low = PROB[s, h, rows, : hi - lo]
                prob = prob_low.astype(F32)
                term = prob * grad_prob
                level = jnp.sum(term, axis=-1, keepdims=True)
                grad = term - prob * level + GLB[s, h, rows, lo:hi].astype(F32)
                GLB[s, h, rows, lo:hi] = grad.astype(BF16)
                GVF[lo:hi, :] += dot_tn(prob_low, cot)
            grad_raw = GLB[s, h]
            GQF[...] += dot_nn(grad_raw, K[all_rows, :] * pick)
            GKF[...] += dot_tn(grad_raw, Q[all_rows, :] * pick)
            for job in between[h]:
                job()
        store = local(GLB.at[s], r_["glin_out"].at[s], 2 + s)
        low_q = (GQF[...] * 0.125).astype(BF16)
        low_k = (GKF[...] * 0.125).astype(BF16)
        low_v = GVF[...].astype(BF16)
        GP[all_rows, :EDGE] = low_q[:, :EDGE]
        GP[all_rows, EDGE:PAIR] = low_q[:, EDGE:] + low_v[:, :EDGE]
        GP[all_rows, PAIR : 3 * EDGE] = low_v[:, EDGE:]
        GP[all_rows, 3 * EDGE :] = low_k
        SMG[8:9, :PAIR] += jnp.sum(low_q.astype(F32), axis=0, keepdims=True)
        SMG[9:10, :PAIR] += jnp.sum(low_v.astype(F32), axis=0, keepdims=True)

        def product(rows):
            return dot_nt(GP[rows, :], WA[:, : 5 * EDGE])

        return store, Reduction(2, s, product)

    def token_grads(s, total):
        def body(r, carry):
            rows = token_rows(s, r)
            GT[rows, :] = (GS[s, pl.ds(r, TILE), :] + total.tile(r)).astype(BF16)
            return carry

        tile_loop(half, body, 0)
        return share(GT, s)

    class Scatter:
        def __init__(self, tag, fill):
            self.stage, self.yr = r_["ST" + tag], r_["YR" + tag]
            self.zs, self.zr = r_["ZS" + tag], r_["ZR" + tag]
            fill(self.stage)
            self.y_in = [
                wires.send(self.stage.at[1 - y, zto[k]], self.yr.at[zto[k]], y_dev)
                for k in (1, 2, 3, 0)
            ]
            self.sent = []

        def block(self, index):
            return self.stage[y, index].astype(F32) + self.yr[index].astype(F32)

        def along(self, k):
            self.y_in[k - 1].wait_recv()
            self.zs[k - 1] = self.block(zto[k]).astype(BF16)
            self.sent.append(wires.send(self.zs.at[k - 1], self.zr.at[k - 1], z_dev[k]))

        def along_all(self):
            for k in range(1, Z):
                self.along(k)

        def finish(self):
            self.y_in[Z - 1].wait_recv()
            total = self.block(z)
            for k in range(1, Z):
                self.sent[k - 1].wait_recv()
                total = total + self.zr[k - 1].astype(F32)
            return total

    def fill_square(left, right):
        def fill(stage):
            part = D // 2
            for i in range(2):
                product = dot_tn(left[:, i * part : (i + 1) * part], right[...]).astype(BF16)
                for j in range(part // SH):
                    index = i * (part // SH) + j
                    stage[index % Y, index // Y] = product[j * SH : (j + 1) * SH, :]

        return fill

    def fill_blocks(stage, at, product):
        wide = product.shape[1]
        for index in range(Z * Y):
            stage[index % Y, index // Y, :, at : at + wide] = product[index * SH : (index + 1) * SH, :]

    def fill_first(stage):
        fill_blocks(stage, 0, dot_tn(tok[...], GP[:, : 3 * EDGE]).astype(BF16))

    def fill_second(stage):
        keys, outs = dot_tn(tok[...], GP[:, 3 * EDGE :]), r_["OG"]
        fill_blocks(stage, 0, keys[:, :EDGE].astype(BF16))
        fill_blocks(stage, EDGE, (keys[:, EDGE:] + outs[:, :EDGE]).astype(BF16))
        fill_blocks(stage, PAIR, outs[:, EDGE:].astype(BF16))

    def pass_on(gather, step):
        return lambda: gather.forward(step)

    store_l0, parts0 = attend(0, ((), (pass_on(gather_u, 0),), (pass_on(gather_d, 0),)))
    wo_x.wait_recv()
    wo_d = wires.send(WO.at[1], WO.at[2], c_dev)
    store_l1, parts1 = attend(1, ((pass_on(gather_u, 1),), (pass_on(gather_d, 1),), ()))
    gather_u.forward(2)
    wo_core.wait_recv()
    wo_d.wait_recv()
    normed0 = out_project(0, parts0)
    gather_d.forward(2)
    normed1 = out_project(1, parts1)
    gather_u.finish()
    normed0.wait_recv()
    feed_up(0)
    normed1.wait_recv()
    feed_up(1)
    gather_d.finish()
    down0 = feed_down(0)
    down1 = feed_down(1)
    down0.cross()
    down0.wait()
    down1.cross()
    branch0, mix0 = norm_two(0, down0)
    branch0.wait_recv()
    back0 = feed_back(0)
    back0.cross()
    down1.wait()
    branch1, mix1 = norm_two(1, down1)
    branch1.wait_recv()
    scatter_d = Scatter("D", fill_square(BR, ACT))
    back1 = feed_back(1)
    scatter_u = Scatter("U", fill_square(NORMED, GH))
    scatter_d.along(1)
    back0.wait()
    back1.cross()
    attn0 = norm_one_back(0, back0)
    scatter_d.along(2)
    attn0.wait_recv()
    store_g0, token0 = attend_back(0, ((), (), ()))
    token0.cross()
    scatter_d.along(3)
    back1.wait()
    attn1 = norm_one_back(1, back1)
    scatter_u.along(1)
    attn1.wait_recv()
    r_["OG"][...] = dot_tn(GAT[...], CTXF[...])

    def pass_up(step):
        return lambda: scatter_u.along(step)

    store_g1, token1 = attend_back(1, ((), (pass_up(2),), (pass_up(3),)))
    small_core = wires.send(SMG, SMR.at[0], c_dev)
    scatter_f = Scatter("F", fill_first)
    small_core.wait_recv()
    upper = lax.broadcasted_iota(jnp.int32, SMG.shape, 0) < 8
    SMS[0] = SMG[...] + jnp.where(upper, SMR[0], 0.0)
    small_y = wires.send(SMS.at[0], SMR.at[1], y_dev)
    scatter_g = Scatter("G", fill_second)
    token0.wait()
    token1.cross()
    share0 = token_grads(0, token0)
    mix0.wait_recv()
    mix1.wait_recv()
    store_mix = local(MIX, r_["mixed"], 4)
    small_y.wait_recv()
    SMS[1] = SMS[0] + SMR[1]
    small_z = [wires.send(SMS.at[1], SMR.at[1 + k], z_dev[k]) for k in range(1, Z)]
    scatter_f.along_all()
    r_["gd"][...] = scatter_d.finish()
    r_["gu"][...] = scatter_u.finish()
    token1.wait()
    share1 = token_grads(1, token1)
    scatter_g.along_all()
    small_total = SMS[1]
    for k in range(1, Z):
        small_z[k - 1].wait_recv()
        small_total = small_total + SMR[1 + k]
    SMV[...] = small_total

    def own(first, count, width, start=0):
        value = SMV[first : first + count, start : start + width]
        for i in range(1, Z * Y):
            here = SMV[first : first + count, start + i * width : start + (i + 1) * width]
            value = jnp.where(dpi == i, here, value)
        return value

    r_["ggains"][...] = own(0, 2, SH)
    r_["gshifts"][...] = own(2, 4, SH)
    r_["ghbias"][0:1] = own(8, 1, piece)
    r_["ghbias"][1:2] = own(9, 1, piece, PAIR - C)
    r_["gfbias"][...] = own(10, 1, SH)
    share0.wait_recv()
    share1.wait_recv()
    store_gt = local(GT, r_["gtok"], 5)
    first = scatter_f.finish()
    r_["ga"][0] = first[:, :C]
    r_["ga"][2] = first[:, C:]
    second = scatter_g.finish()
    r_["ga"][1] = second[:, :C]
    r_["go"][...] = jnp.transpose(second[:, C:])
    for copy in (store_l0, store_l1, store_g0, store_g1, store_mix, store_gt):
        copy.wait()
    wires.drain_all()


def pass_kernel(count, *refs):
    sources, targets = refs[:count], refs[count : 2 * count]
    held, sem = refs[2 * count : 3 * count], refs[3 * count]
    loads = [
        pltpu.make_async_copy(sources[i], held[i], sem.at[i]) for i in range(count)
    ]
    stores = [
        pltpu.make_async_copy(held[i], targets[i], sem.at[count + i]) for i in range(count)
    ]
    for copy in loads:
        copy.start()
    for load, store in zip(loads, stores, strict=True):
        load.wait()
        store.start()
    for copy in stores:
        copy.wait()


def pass_through(arrays):
    count = len(arrays)
    far = pl.BlockSpec(memory_space=pl.ANY)
    return pl.pallas_call(
        functools.partial(pass_kernel, count),
        out_shape=tuple(jax.ShapeDtypeStruct(a.shape, a.dtype) for a in arrays),
        in_specs=[far] * count,
        out_specs=(far,) * count,
        scratch_shapes=[pltpu.VMEM(a.shape, a.dtype) for a in arrays]
        + [pltpu.SemaphoreType.DMA((2 * count,))],
    )(*arrays)


def fused_shards(
    tokens, segments, logits_in, w_qkv, w_out, w_up, w_down,
    head_bias, ff_bias, norm_gains, shift_biases, grad_out, grad_logits,
):
    rows, D = tokens.shape
    seqs, L = segments.shape
    HEADS = logits_in.shape[1]
    SH, unused, C = w_qkv.shape
    FF = w_up.shape[1]
    HD = C // HEADS
    half = L // 2
    width = max(D, FF)
    dma = pltpu.SemaphoreType.DMA
    vm = pltpu.VMEM
    inputs = {
        "tok_far": tokens, "wa": jnp.transpose(w_qkv, (1, 0, 2)), "wo": w_out, "wu": w_up,
        "wd": w_down.T, "hbias": head_bias, "fbias": ff_bias[None], "gains": norm_gains,
        "shifts": shift_biases, "seg": segments,
        "gout": grad_out, "lin": logits_in, "gl": grad_logits,
    }
    shape = jax.ShapeDtypeStruct
    outputs = {
        "mixed": shape((rows, D), BF16),
        "logits_out": shape(logits_in.shape, BF16),
        "gtok": shape((rows, D), BF16),
        "glin_out": shape(logits_in.shape, BF16),
        "ga": shape((3, SH, C), F32),
        "go": shape((C, SH), F32),
        "gu": shape((SH, FF), F32),
        "gd": shape((SH, FF), F32),
        "ghbias": shape(head_bias.shape, F32),
        "gfbias": shape((1,) + ff_bias.shape, F32),
        "ggains": shape(norm_gains.shape, F32),
        "gshifts": shape(shift_biases.shape, F32),
    }
    scratch = {
        "tok": vm((rows, D), BF16),
        "WA": vm((D, 6 * EDGE), BF16), "PK": vm((SH, 6 * EDGE), BF16), "WU": vm((D, FF), BF16),
        "WD": vm((D, FF), BF16), "BLEND": vm((16, EDGE), F32),
        "SMB": vm((16, EDGE), BF16), "SM": vm((16, Z * Y * EDGE), BF16),
        "SMV": vm((16, width), F32), "HBV": vm((16, 4 * EDGE), F32), "WO": vm((3, D, 2 * EDGE), BF16),
        "GOUT": vm((seqs, half, D), BF16),
        "Q": vm((rows, 2 * EDGE), BF16), "K": vm((rows, 2 * EDGE), BF16), "V": vm((rows, 2 * EDGE), BF16),
        "LIN": vm(logits_in.shape, BF16), "GLB": vm(logits_in.shape, BF16),
        "PROB": vm((seqs, HEADS, L, 3 * EDGE), BF16), "BIAS": vm((L, 3 * EDGE), F32),
        "CTXF": vm((rows, 2 * EDGE), BF16), "CTXR": vm((3, seqs, half, 2 * EDGE), BF16),
        "NORMED": vm((rows, D), BF16), "ACT": vm((rows, FF), BF16), "DG": vm((rows, FF), F32),
        "BR": vm((rows, D), BF16), "GH": vm((rows, FF), BF16), "GAT": vm((rows, D), BF16),
        "GC": vm((L, 2 * EDGE), BF16), "MIX": vm((rows, D), BF16), "GT": vm((rows, D), BF16),
        "XH1": vm((seqs, half, D), F32), "R1": vm((seqs, half, EDGE), F32),
        "GS": vm((seqs, half, D), F32), "HB": vm((CHUNK, width), F32),
        "OWN": vm((seqs, half, D), F32), "CS": vm((seqs, half, D), BF16),
        "CR": vm((seqs, half, D), BF16), "XS": vm((seqs, half, D), BF16),
        "XR": vm((3, seqs, half, D), BF16), "GP": vm((rows, 5 * EDGE), BF16), "OG": vm((D, 2 * EDGE), F32),
        "GQF": vm((L, 2 * EDGE), F32), "GKF": vm((L, 2 * EDGE), F32), "GVF": vm((L, 2 * EDGE), F32),
        "SMG": vm((16, width), F32), "SMS": vm((2, 16, width), F32), "SMR": vm((5, 16, width), F32),
        "send_sem": dma((COPIES,)), "recv_sem": dma((COPIES,)), "local_sem": dma((8,)),
    }
    for tag in "UDFG":
        block = (SH, FF if tag in "UD" else 3 * EDGE)
        scratch["ST" + tag] = vm((Y, Z) + block, BF16)
        scratch["YR" + tag] = vm((Z,) + block, BF16)
        scratch["ZS" + tag] = vm((Z - 1,) + block, BF16)
        scratch["ZR" + tag] = vm((Z - 1,) + block, BF16)
    near, far = pl.BlockSpec(memory_space=pltpu.VMEM), pl.BlockSpec(memory_space=pl.ANY)
    distant = ("tok_far", "gout", "lin", "gl", "mixed", "logits_out", "gtok", "glin_out")
    names = (*inputs, *outputs, *scratch)
    dims = (L, HEADS, HD, D, FF, C, SH)
    results = pl.pallas_call(
        functools.partial(layer_kernel, names, dims),
        out_shape=tuple(outputs.values()),
        in_specs=[far if name in distant else near for name in inputs],
        out_specs=tuple(far if name in distant else near for name in outputs),
        scratch_shapes=list(scratch.values()),
        compiler_params=pltpu.CompilerParams(
            collective_id=0, has_side_effects=True, vmem_limit_bytes=66 * 1000 * 1000
        ),
    )(*inputs.values())
    mixed, logits_out, gtok, glin, ga, go, gu, gd, ghbias, gfbias, ggains, gshifts = pass_through(
        results
    )
    return (
        mixed,
        logits_out,
        gtok,
        glin,
        jnp.transpose(ga, (1, 0, 2)),
        go,
        gu,
        gd.T,
        ghbias,
        gfbias[0],
        ggains,
        gshifts,
    )


def solution(mesh):
    body = fused_shards if mesh.shape["dp"] == Z * Y and mesh.shape["mp"] == 2 * CORES else shards
    return jax.shard_map(
        body,
        mesh=mesh,
        in_specs=(
            P("dp", None),
            P("dp", None),
            P("dp", "mp", None, None),
            P("dp", None, "mp"),
            P("mp", "dp"),
            P("dp", "mp"),
            P("mp", "dp"),
            P(None, ("mp", "dp")),
            P(("mp", "dp")),
            P(None, "dp"),
            P(None, "dp"),
            P("dp", None),
            P("dp", "mp", None, None),
        ),
        out_specs=(
            P("dp", None),
            P("dp", "mp", None, None),
            P("dp", None),
            P("dp", "mp", None, None),
            P("dp", None, "mp"),
            P("mp", "dp"),
            P("dp", "mp"),
            P("mp", "dp"),
            P(None, ("mp", "dp")),
            P(("mp", "dp")),
            P(None, "dp"),
            P(None, "dp"),
        ),
        check_vma=False,
    )
```

```python
import functools
import types

import jax
import jax.numpy as jnp
from jax import lax
from jax.experimental import pallas as pl
from jax.experimental.pallas import tpu as pltpu
from jax.sharding import PartitionSpec as P

MB = 2
MESH = pl.DeviceIdType.MESH
F32 = jnp.float32
BF16 = jnp.bfloat16

epsilon = 1e-05
masked_value = -10000.0


def norm_rows(hidden, gain, shift):
    center = hidden - jnp.mean(hidden, axis=-1, keepdims=True)
    spread = jnp.mean(center * center, axis=-1, keepdims=True)
    return center * lax.rsqrt(spread + epsilon) * gain + shift


def gelu_exact(value):
    return 0.5 * value * (1.0 + lax.erf(value * 0.7071067811865476))


def add_trees(first_tree, second_tree):
    if first_tree is None:
        return second_tree
    return jax.tree.map(jnp.add, first_tree, second_tree)


def micro_step(whole, block_tokens, block_segments, block_logits, block_grad, block_grad_logits):
    qkv_weight, out_weight, up_weight, down_weight, bias_heads, bias_hidden, gains, shifts = whole
    seq_count = block_segments.shape[0]
    length = block_segments.shape[1]
    feature = block_tokens.shape[1]
    row_count = block_tokens.shape[0]
    local_heads = block_logits.shape[1]
    flat_qkv = qkv_weight.reshape(feature, -1)
    local_cols = flat_qkv.shape[1] // 3
    head_size = local_cols // local_heads
    gain_rows = gains.astype(jnp.float32)
    shift_rows = shifts.astype(jnp.float32)
    head_rows = bias_heads.astype(jnp.float32)
    shape_heads = (seq_count, length, local_heads, head_size)
    token_float = block_tokens.astype(jnp.float32)
    projected = jnp.dot(block_tokens, flat_qkv, preferred_element_type=jnp.float32)
    query = (projected[:, :local_cols] + head_rows[0]).astype(jnp.bfloat16).reshape(shape_heads)
    keys = projected[:, local_cols : 2 * local_cols].astype(jnp.bfloat16).reshape(shape_heads)
    values = (
        (projected[:, 2 * local_cols :] + head_rows[1]).astype(jnp.bfloat16).reshape(shape_heads)
    )
    same = block_segments[:, :, None] == block_segments[:, None, :]
    mask = jnp.where(same, 0.0, masked_value).astype(jnp.float32)[:, None]
    incoming = block_logits.astype(jnp.float32)
    raw = (
        jnp.einsum("sqhd,skhd->shqk", query, keys, preferred_element_type=jnp.float32) * 0.125
        + incoming
    )
    shifted = raw + mask
    top = jnp.max(shifted, axis=-1, keepdims=True)
    expo = jnp.exp(shifted - top)
    total = jnp.sum(expo, axis=-1, keepdims=True)
    log_total = top + jnp.log(total)
    context = jnp.einsum(
        "shqk,skhd->sqhd",
        (expo / total).astype(jnp.bfloat16),
        values,
        preferred_element_type=jnp.float32,
    )
    context = context.reshape(row_count, local_cols).astype(jnp.bfloat16)
    attn_total = lax.psum(jnp.dot(context, out_weight, preferred_element_type=jnp.float32), "mp")
    first_pre = attn_total + shift_rows[0] + token_float
    normed = norm_rows(first_pre, gain_rows[0], shift_rows[1]).astype(jnp.bfloat16)
    hidden_pre = jnp.dot(
        normed, up_weight, preferred_element_type=jnp.float32
    ) + bias_hidden.astype(jnp.float32)
    activated = gelu_exact(hidden_pre).astype(jnp.bfloat16)
    ffn_total = lax.psum(jnp.dot(activated, down_weight, preferred_element_type=jnp.float32), "mp")
    second_pre = ffn_total + shift_rows[2] + normed.astype(jnp.float32)
    cotangent = block_grad.astype(jnp.float32)
    mixed_part = norm_rows(second_pre, gain_rows[1], shift_rows[3]).astype(jnp.bfloat16)
    unused_second, second_pull = jax.vjp(norm_rows, second_pre, gain_rows[1], shift_rows[3])
    grad_second, grad_gain_two, grad_shift_two = second_pull(cotangent)
    branch_part = grad_second.astype(jnp.bfloat16)
    grad_bias_two = jnp.sum(branch_part.astype(jnp.float32), axis=0)
    grad_down = jnp.einsum("rf,rd->fd", activated, branch_part, preferred_element_type=jnp.float32)
    grad_act = jnp.einsum("rd,fd->rf", branch_part, down_weight, preferred_element_type=jnp.float32)
    unused_gelu, gelu_pull = jax.vjp(gelu_exact, hidden_pre)
    grad_hidden = gelu_pull(grad_act)[0].astype(jnp.bfloat16)
    grad_bias_hidden = jnp.sum(grad_hidden.astype(jnp.float32), axis=0)
    grad_up = jnp.einsum("rd,rf->df", normed, grad_hidden, preferred_element_type=jnp.float32)
    hidden_terms = jnp.einsum(
        "rf,df->rd", grad_hidden, up_weight, preferred_element_type=jnp.float32
    )
    grad_normed = grad_second + lax.psum(hidden_terms, "mp")
    unused_first, first_pull = jax.vjp(norm_rows, first_pre, gain_rows[0], shift_rows[1])
    grad_first, grad_gain_one, grad_shift_one = first_pull(grad_normed)
    grad_attn = grad_first.astype(jnp.bfloat16)
    grad_bias_out = jnp.sum(grad_attn.astype(jnp.float32), axis=0)
    grad_out_weight = jnp.einsum(
        "rc,rd->cd", context, grad_attn, preferred_element_type=jnp.float32
    )
    grad_context = jnp.einsum(
        "rd,cd->rc", grad_attn, out_weight, preferred_element_type=jnp.float32
    )
    grad_context = grad_context.astype(jnp.bfloat16).reshape(shape_heads)
    raw_again = (
        jnp.einsum("sqhd,skhd->shqk", query, keys, preferred_element_type=jnp.float32) * 0.125
        + incoming
    )
    prob = jnp.exp(raw_again + mask - log_total)
    grad_prob = jnp.einsum(
        "sqhd,skhd->shqk", grad_context, values, preferred_element_type=jnp.float32
    )
    grad_raw = prob * (
        grad_prob - jnp.sum(prob * grad_prob, axis=-1, keepdims=True)
    ) + block_grad_logits.astype(jnp.float32)
    grad_raw_low = grad_raw.astype(jnp.bfloat16)
    grad_query = (
        jnp.einsum("shqk,skhd->sqhd", grad_raw_low, keys, preferred_element_type=jnp.float32)
        * 0.125
    )
    grad_keys = (
        jnp.einsum("shqk,sqhd->skhd", grad_raw_low, query, preferred_element_type=jnp.float32)
        * 0.125
    )
    grad_values = jnp.einsum(
        "shqk,sqhd->skhd",
        prob.astype(jnp.bfloat16),
        grad_context,
        preferred_element_type=jnp.float32,
    )
    grad_query = grad_query.astype(jnp.bfloat16).reshape(row_count, local_cols)
    grad_keys = grad_keys.astype(jnp.bfloat16).reshape(row_count, local_cols)
    grad_values = grad_values.astype(jnp.bfloat16).reshape(row_count, local_cols)
    grad_proj = jnp.concatenate([grad_query, grad_keys, grad_values], axis=1)
    grad_qkv = jnp.einsum(
        "rd,rc->dc", block_tokens, grad_proj, preferred_element_type=jnp.float32
    ).reshape(qkv_weight.shape)
    grad_heads = jnp.stack(
        [
            jnp.sum(grad_query.astype(jnp.float32), axis=0),
            jnp.sum(grad_values.astype(jnp.float32), axis=0),
        ]
    )
    input_terms = jnp.einsum("rc,dc->rd", grad_proj, flat_qkv, preferred_element_type=jnp.float32)
    grad_inputs = grad_first + lax.psum(input_terms.astype(jnp.bfloat16), "mp").astype(jnp.float32)
    results = (mixed_part, raw.astype(jnp.bfloat16), grad_inputs.astype(jnp.bfloat16), grad_raw_low)
    grads = (
        grad_qkv,
        grad_out_weight,
        grad_up,
        grad_down,
        grad_heads,
        grad_bias_hidden,
        jnp.stack([grad_gain_one, grad_gain_two]),
        jnp.stack([grad_bias_out, grad_shift_one, grad_bias_two, grad_shift_two]),
    )
    return (results, grads)


def shards(
    tokens,
    segments,
    logits_in,
    w_qkv,
    w_out,
    w_up,
    w_down,
    head_bias,
    ff_bias,
    norm_gains,
    shift_biases,
    grad_out,
    grad_logits,
):
    seq_count = segments.shape[0] // MB
    row_count = seq_count * segments.shape[1]
    collected = []
    totals = None
    for micro in range(MB):
        whole = (
            lax.all_gather(w_qkv, "dp", axis=0, tiled=True),
            lax.all_gather(w_out, "dp", axis=1, tiled=True),
            lax.all_gather(w_up, "dp", axis=0, tiled=True),
            lax.all_gather(w_down, "dp", axis=1, tiled=True),
            lax.all_gather(head_bias, "dp", axis=1, tiled=True),
            lax.all_gather(ff_bias, "dp", axis=0, tiled=True),
            lax.all_gather(norm_gains, "dp", axis=1, tiled=True),
            lax.all_gather(shift_biases, "dp", axis=1, tiled=True),
        )
        first_row = micro * row_count
        first_seq = micro * seq_count
        results, grads = micro_step(
            whole,
            tokens[first_row : first_row + row_count],
            segments[first_seq : first_seq + seq_count],
            logits_in[first_seq : first_seq + seq_count],
            grad_out[first_row : first_row + row_count],
            grad_logits[first_seq : first_seq + seq_count],
        )
        totals = add_trees(totals, grads)
        collected.append(results)
    totals = (
        lax.psum_scatter(totals[0], "dp", scatter_dimension=0, tiled=True),
        lax.psum_scatter(totals[1], "dp", scatter_dimension=1, tiled=True),
        lax.psum_scatter(totals[2], "dp", scatter_dimension=0, tiled=True),
        lax.psum_scatter(totals[3], "dp", scatter_dimension=1, tiled=True),
        lax.psum_scatter(totals[4], "dp", scatter_dimension=1, tiled=True),
        lax.psum_scatter(totals[5], "dp", scatter_dimension=0, tiled=True),
        lax.psum_scatter(totals[6], "dp", scatter_dimension=1, tiled=True),
        lax.psum_scatter(totals[7], "dp", scatter_dimension=1, tiled=True),
    )
    mixed = jnp.concatenate([item[0] for item in collected], axis=0)
    logits_out = jnp.concatenate([item[1] for item in collected], axis=0)
    grad_tokens = jnp.concatenate([item[2] for item in collected], axis=0)
    grad_logits_in = jnp.concatenate([item[3] for item in collected], axis=0)
    return (
        mixed,
        logits_out,
        grad_tokens,
        grad_logits_in,
        totals[0],
        totals[1],
        totals[2],
        totals[3],
        totals[4],
        totals[5],
        totals[6],
        totals[7],
    )


Z, Y, CORES = 4, 2, 2
TILE = 32
EDGE = 128
CHUNK = 256
SENDS, ARRIVALS, LOADS = 144, 116, 16


def dot_nn(a, b):
    return lax.dot_general(a, b, (((1,), (0,)), ((), ())), preferred_element_type=F32)


def dot_nt(a, b):
    return lax.dot_general(a, b, (((1,), (1,)), ((), ())), preferred_element_type=F32)


def dot_tn(a, b):
    return lax.dot_general(a, b, (((0,), (0,)), ((), ())), preferred_element_type=F32)


def fold_rows(value):
    rows, cols = value.shape
    return jnp.sum(value.reshape(rows // 8, 8, cols), axis=0)


class Wires:
    def __init__(self, send_sem, recv_sem):
        self.send_sem, self.recv_sem, self.sent, self.drained = send_sem, recv_sem, [], []
        self.slots = 0

    def take(self, count):
        self.slots += count
        return self.slots - count

    def describe(self, src, dst, device, out, into):
        return pltpu.make_async_remote_copy(
            src_ref=src,
            dst_ref=dst,
            send_sem=self.send_sem.at[out],
            recv_sem=self.recv_sem.at[into],
            device_id=device,
            device_id_type=MESH,
        )

    def send(self, src, dst, device, into=None):
        copy = self.describe(
            src, dst, device, len(self.sent), self.take(1) if into is None else into
        )
        copy.start()
        self.sent.append(copy)
        return copy

    def send_if(self, condition, src, dst, device, into):
        copy = self.describe(src, dst, device, len(self.sent), into)
        pl.when(condition)(copy.start)
        self.sent.append((copy, condition))

    def arrived(self, ref, device, into):
        self.describe(ref, ref, device, 0, into).wait_recv()

    def drain(self, copy):
        copy.wait_send()
        self.drained.append(copy)

    def drain_all(self):
        for copy in self.sent:
            if isinstance(copy, tuple):
                pl.when(copy[1])(copy[0].wait_send)
            elif not any(copy is done for done in self.drained):
                copy.wait_send()


def layer_kernel(names, dims, *refs):
    r_ = types.SimpleNamespace(**dict(zip(names, refs, strict=True)))
    L, HEADS, HD, D, FF, C, SH = dims
    seqs = 2
    half = L // 2
    tok, seg, GOUT = r_.tok, r_.seg, r_.GOUT
    WA, WU, WD, WO, SMV = r_.WA, r_.WU, r_.WD, r_.WO, r_.SMV
    Q, K, V, LIN, GLB, PROB = r_.Q, r_.K, r_.V, r_.logits_out, r_.glin_out, r_.PROB
    BIAS, CTXF, CTXR = r_.BIAS, r_.CTXF, r_.CTXR
    NORMED, ACT, DG, BR, GH, GAT = r_.NORMED, r_.ACT, r_.DG, r_.BR, r_.GH, r_.GAT
    GC, MIX, GT, XH1, R1, GS = r_.GC, r_.mixed, r_.gtok, r_.XH1, r_.R1, r_.GS
    HB, CS, CR, XS, XR = r_.HB, r_.CS, r_.CR, r_.XS, r_.XR
    OWN, GP = r_.OWN, r_.GP
    GQF, GKF, GVF = r_.GQF, r_.GKF, r_.GVF
    SMG, SMS, SMR = r_.SMG, r_.SMS, r_.SMR
    local_sem = r_.local_sem

    dpi, mpi = lax.axis_index("dp"), lax.axis_index("mp")
    z, y = lax.div(dpi, Y), lax.rem(dpi, Y)
    x, core = lax.div(mpi, CORES), lax.rem(mpi, CORES)
    wires = Wires(r_.send_sem, r_.recv_sem)

    def dev(zz, yy, xx, cc):
        return {"dp": zz * Y + yy, "mp": xx * CORES + cc}

    zto = [lax.rem(z + k, Z) for k in range(Z)]
    zfrom = [lax.rem(z - k + Z, Z) for k in range(Z)]
    z_dev = [dev(zto[k], y, x, core) for k in range(Z)]
    y_dev = dev(z, 1 - y, x, core)
    c_dev = dev(z, y, x, 1 - core)
    x_dev = dev(z, y, 1 - x, core)
    d_dev = dev(z, y, 1 - x, 1 - core)

    barrier = pltpu.get_barrier_semaphore()
    friends = z_dev[1:] + [y_dev, c_dev, x_dev, d_dev]
    for friend in friends:
        pl.semaphore_signal(barrier, inc=1, device_id=friend, device_id_type=MESH)

    locals_used = []

    def local(src, dst):
        copy = pltpu.make_async_copy(src, dst, local_sem.at[len(locals_used)])
        copy.start()
        locals_used.append(copy)
        return copy

    def rows_of(index):
        return pl.ds(pl.multiple_of(index * SH, SH), SH)

    load_first = [local(r_.wa_far, r_.wa), local(r_.wo_far, r_.wo)]
    load_vecs = [
        local(r_.hbias_far, r_.hbias),
        local(r_.fbias_far, r_.fbias),
        local(r_.gains_far, r_.gains),
        local(r_.shifts_far, r_.shifts),
    ]
    load_up = local(r_.wu, WU.at[rows_of(dpi), :])
    load_down = local(r_.wd, WD.at[rows_of(dpi), :])
    load_tok = local(r_.tok_far, tok)
    load_seg = local(r_.seg_far, seg)
    load_lin = [local(r_.lin.at[s], LIN.at[s]) for s in range(seqs)]
    load_gout = [
        local(
            r_.gout.at[pl.ds(pl.multiple_of(s * L + core * half, half), half), :],
            GOUT.at[s],
        )
        for s in range(seqs)
    ]
    load_gl = [local(r_.gl.at[s], GLB.at[s]) for s in range(seqs)]
    def iotas(rows, cols):
        down = lax.broadcasted_iota(jnp.int32, (rows, cols), 0)
        return down, lax.broadcasted_iota(jnp.int32, (rows, cols), 1)

    def shifted(rows, cols, by):
        down, over = iotas(rows, cols)
        return jnp.where(over - down == by, 1.0, 0.0).astype(BF16)

    PAIR = 2 * EDGE
    wa, here = r_.wa, rows_of(dpi)
    even, odd = shifted(C, PAIR, 0), shifted(C, PAIR, PAIR - C)
    for copy in load_first:
        copy.wait()
    out_low = dot_nt(shifted(SH, SH, 0), r_.wo[...]).astype(BF16)
    for at, first, second in ((0, wa[0], wa[2]), (3 * EDGE, wa[1], out_low)):
        first, second = dot_nn(first, even), dot_nn(second, odd)
        WA[here, at : at + EDGE] = first[:, :EDGE].astype(BF16)
        WA[here, at + EDGE : at + PAIR] = (first[:, EDGE:] + second[:, :EDGE]).astype(BF16)
        WA[here, at + PAIR : at + 3 * EDGE] = second[:, EDGE:].astype(BF16)

    pl.semaphore_wait(barrier, len(friends))

    near = z - 1 + 2 * lax.div(3 - z, 3)
    last = 3 * (1 - lax.div(z, 2))
    order = [near, 6 - z - near - last, last]

    class Gather:
        def __init__(self, dst, place):
            self.dst, self.place = dst, place
            self.own = dst.at[place(dpi)]
            self.z_in, self.y_in = wires.take(Z), wires.take(Z)

        def along(self):
            for there in order:
                wires.send(self.own, self.own, dev(there, y, x, core), self.z_in + z)

        def across(self):
            wires.send(self.own, self.own, y_dev, self.y_in + z)

        def forward(self, step):
            origin = order[step]
            block = self.dst.at[self.place(origin * Y + y)]
            wires.arrived(block, y_dev, self.z_in + origin)
            wires.send(block, block, y_dev, self.y_in + origin)

        def finish(self):
            for origin in range(Z):
                block = self.dst.at[self.place(origin * Y + 1 - y)]
                wires.arrived(block, y_dev, self.y_in + origin)

    class Line(Gather):
        turns = True

        def block(self, origin):
            return self.dst.at[self.place(jnp.clip(origin, 0, Z - 1) * Y + y)]

        def push(self, src, origin, held, side):
            block = self.block(origin)
            room, there = ((z < Z - 1, z + 1), (z > 0, z - 1))[side]
            going = room if held is None else jnp.logical_and(room, held)
            device = dev(jnp.clip(there, 0, Z - 1), y, x, core)
            slot = self.z_in + jnp.clip(origin, 0, Z - 1)
            wires.send_if(going, src, block, device, slot)

        def start(self):
            for side in range(2):
                self.push(self.own, z, None, side)

        def step(self, hop):
            for side, origin, held in ((0, z - hop, z >= hop), (1, z + hop, z + hop < Z)):
                block = self.block(origin)
                slot = jnp.clip(origin, 0, Z - 1)

                @pl.when(held)
                def arrive():
                    wires.arrived(block, y_dev, self.z_in + slot)

                self.push(block, origin, held, side)
                if self.turns:
                    wires.send_if(held, block, block, y_dev, self.y_in + slot)

    class PairLine(Line):
        turns = False

        def __init__(self, dst, place, place_pair):
            Gather.__init__(self, dst, place)
            self.place_pair = place_pair

        def block(self, origin):
            return self.dst.at[self.place_pair(jnp.clip(origin, 0, Z - 1))]

        def meet(self):
            wires.arrived(self.dst.at[self.place(z * Y + 1 - y)], y_dev, self.y_in + z)
            self.own = self.block(z)
            self.start()

    def rows_of(index):
        return pl.ds(pl.multiple_of(index * SH, SH), SH)

    def lanes_of(start, stop):
        return lambda index: (rows_of(index), slice(start, stop))

    def by_lanes(index):
        return (slice(None), pl.ds(pl.multiple_of(index * EDGE, EDGE), EDGE))

    SM = r_.SM
    gather_a = Line(WA, lanes_of(0, 3 * EDGE))
    gather_b = Line(WA, lanes_of(3 * EDGE, 6 * EDGE))
    gather_s = Gather(SM, by_lanes)
    gather_u = Line(WU, lanes_of(0, FF))
    cut = FF - PAIR
    gather_d = Line(WD, lanes_of(0, cut))
    gather_e = PairLine(
        WD,
        lanes_of(cut, FF),
        lambda i: (pl.ds(pl.multiple_of(i * Y * SH, Y * SH), Y * SH), slice(cut, FF)),
    )

    gather_a.start()
    gather_b.start()
    gather_a.across()
    gather_b.across()

    for copy in load_vecs:
        copy.wait()
    blend = r_.BLEND
    blend[...] = jnp.zeros_like(blend)
    blend[0:2, :SH] = r_.gains[...].astype(F32)
    blend[2:6, :SH] = r_.shifts[...].astype(F32)
    piece = r_.hbias.shape[1]
    blend[8:10, :piece] = r_.hbias[...].astype(F32)
    blend[10:11, :SH] = r_.fbias[...].astype(F32)
    SM[by_lanes(dpi)] = blend[...].astype(BF16)
    gather_s.along()
    gather_s.across()
    gather_a.step(1)
    gather_b.step(1)
    for i in range(Z * Y):
        rows = slice(i * EDGE, (i + 1) * EDGE)
        down, over = iotas(EDGE, GH.shape[1])
        GH[rows, :] = jnp.where((over - down == i * SH) & (down < SH), 1.0, 0.0).astype(BF16)
        down, over = iotas(EDGE, 2 * PAIR)
        gap = i * piece + jnp.where(over < PAIR, 0, PAIR + PAIR - C)
        ACT[rows, : 2 * PAIR] = jnp.where(
            (over - down == gap) & (down < piece), 1.0, 0.0
        ).astype(BF16)

    gather_a.step(2)
    gather_b.step(2)
    gather_a.step(3)
    gather_b.step(3)
    load_up.wait()
    load_down.wait()
    gather_u.start()
    for step in range(Z - 1):
        gather_s.forward(step)
    gather_a.finish()
    gather_b.finish()
    gather_s.finish()
    gather_u.across()
    gather_e.across()
    outer = WA.at[:, 4 * EDGE : 6 * EDGE]
    wo_core = wires.send(outer, WO.at[0], c_dev)
    wo_x = wires.send(outer, WO.at[1], x_dev)

    SMV[...] = dot_nn(SM[...], GH[...])
    r_.HBV[...] = dot_nn(SM[...], ACT[:, : 2 * PAIR])
    SMG[...] = jnp.zeros_like(SMG)

    def vec(row, width=D):
        return SMV[row : row + 1, :width]

    def project(i, carry):
        rows = pl.ds(pl.multiple_of(i * CHUNK, CHUNK), CHUNK)
        block = tok[rows, :]
        HBV = r_.HBV
        Q[rows, :] = (dot_nn(block, WA[:, :PAIR]) + HBV[8:9, :PAIR]).astype(BF16)
        V[rows, :] = (dot_nn(block, WA[:, EDGE : 3 * EDGE]) + HBV[9:10, PAIR:]).astype(BF16)
        K[rows, :] = dot_nn(block, WA[:, 3 * EDGE : 5 * EDGE]).astype(BF16)
        return carry

    gather_u.step(1)
    gather_d.start()
    load_tok.wait()
    load_seg.wait()
    lax.fori_loop(0, seqs * L // CHUNK, project, 0)

    lanes = lax.broadcasted_iota(jnp.int32, (1, PAIR), 1)

    def head_mask(h, start=0):
        inside = (lanes >= start + h * HD) & (lanes < start + (h + 1) * HD)
        return jnp.where(inside, 1.0, 0.0).astype(BF16)

    blocks = L // EDGE
    windows = [(max(b - 1, 0) * EDGE, min(b + 2, blocks) * EDGE) for b in range(blocks)]

    def half_of(s, which):
        return pl.ds(pl.multiple_of(s * L + which * half, half), half)

    def mine(s):
        return half_of(s, core)

    def theirs(s):
        return half_of(s, 1 - core)

    def attend(s, between):
        base = s * L
        ids = seg[s : s + 1, :].astype(F32)
        tall = jnp.transpose(jnp.broadcast_to(ids, (EDGE, L)))
        for b, (lo, hi) in enumerate(windows):
            for j in range((hi - lo) // EDGE):
                near = ids[:, lo + j * EDGE : lo + (j + 1) * EDGE]
                same = tall[b * EDGE : (b + 1) * EDGE, :] == near
                BIAS[b * EDGE : (b + 1) * EDGE, j * EDGE : (j + 1) * EDGE] = jnp.where(
                    same, 0.0, masked_value
                ).astype(F32)
        GQF[...] = jnp.zeros_like(GQF)
        load_lin[s].wait()

        for h in range(HEADS):
            pick, pick_v = head_mask(h), head_mask(h, PAIR - C)
            for b, (lo, hi) in enumerate(windows):
                rows = slice(b * EDGE, (b + 1) * EDGE)
                query = Q[base + b * EDGE : base + (b + 1) * EDGE, :] * pick
                score = dot_nt(query, K[base : base + L, :])
                raw = score * 0.125 + LIN[s, h, rows, :].astype(F32)
                LIN[s, h, rows, :] = raw.astype(BF16)
                near = raw[:, lo:hi] + BIAS[rows, : hi - lo]
                top = jnp.max(near, axis=-1, keepdims=True)
                expo = jnp.exp(near - top)
                norm = 1.0 / jnp.sum(expo, axis=-1, keepdims=True)
                prob = (expo * norm).astype(BF16)
                PROB[s, h, rows, : hi - lo] = prob
                GQF[rows, :] += dot_nn(prob, V[base + lo : base + hi, :] * pick_v)
            for job in between[h]:
                job()
        CTXF[base : base + L, :] = GQF[...].astype(BF16)
        parts = [
            wires.send(CTXF.at[theirs(s), :], CTXR.at[0, s], c_dev),
            wires.send(CTXF.at[mine(s), :], CTXR.at[1, s], x_dev),
            wires.send(CTXF.at[theirs(s), :], CTXR.at[2, s], d_dev),
        ]
        return parts

    def tile_loop(count, body, init):
        def step(i, carry):
            start = pl.multiple_of(i * 2 * TILE, 2 * TILE)
            return body(start + TILE, body(start, carry))

        return lax.fori_loop(0, count // (2 * TILE), step, init)

    def token_rows(s, r):
        return pl.ds(pl.multiple_of(s * L + core * half + r, TILE), TILE)

    def normalize(value):
        center = value - jnp.mean(value, axis=-1, keepdims=True)
        spread = jnp.mean(center * center, axis=-1, keepdims=True)
        scale = lax.rsqrt(spread + epsilon)
        return center * scale, scale

    def norm_back(scaled, xhat, scale):
        flat = jnp.mean(scaled, axis=-1, keepdims=True)
        tilt = jnp.mean(scaled * xhat, axis=-1, keepdims=True)
        return scale * (scaled - flat - xhat * tilt)

    def add_small(rows, sums):
        for row, value in zip(rows, sums, strict=True):
            SMG[row : row + 1, :] += jnp.sum(value, axis=0, keepdims=True)

    def share(ref, s):
        return wires.send(ref.at[mine(s), :], ref.at[mine(s), :], c_dev)

    def out_project(s, parts):
        for copy in parts:
            copy.wait_recv()
        HB[...] = dot_nt(CTXF[mine(s), :], outer[...]) + dot_nt(CTXR[0, s], WO[0])
        OWN[s] = dot_nt(CTXR[1, s], WO[1]) + dot_nt(CTXR[2, s], WO[2])

        def body(r, carry):
            at = pl.ds(r, TILE)
            first = (HB[at, :] + OWN[s, at, :]) + vec(2) + tok[token_rows(s, r), :].astype(F32)
            xhat, scale = normalize(first)
            XH1[s, at, :] = xhat
            R1[s, at, :] = jnp.broadcast_to(scale, (TILE, EDGE))
            NORMED[token_rows(s, r), :] = (xhat * vec(0) + vec(3)).astype(BF16)
            return carry

        tile_loop(half, body, 0)
        return share(NORMED, s)

    def feed_up(s):
        def block(i, carry):
            start = s * L + i * CHUNK
            rows = pl.ds(pl.multiple_of(start, CHUNK), CHUNK)
            HB[...] = dot_nn(NORMED[rows, :], WU[...]) + vec(10, FF)

            def body(r, inner):
                to = pl.ds(pl.multiple_of(start + r, TILE), TILE)
                value = HB[pl.ds(r, TILE), :]
                cdf = 0.5 * (1.0 + lax.erf(value * 0.7071067811865476))
                ACT[to, :] = (value * cdf).astype(BF16)
                DG[to, :] = cdf + value * (jnp.exp(-0.5 * value * value) * 0.3989422804014327)
                return inner

            return tile_loop(CHUNK, body, carry)

        lax.fori_loop(0, L // CHUNK, block, 0)

    last_sum = [None] * seqs

    class Reduction:
        def __init__(self, stage, s, product):
            self.stage, self.s = stage, s
            before = last_sum[s]
            if before is not None:
                wires.drain(before.pair)
                wires.drain(before.far)
            last_sum[s] = self
            CS[s] = product(theirs(s)).astype(BF16)
            self.pair = wires.send(CS.at[s], CR.at[s], c_dev)
            OWN[s] = product(mine(s))

        def cross(self):
            s = self.s
            self.pair.wait_recv()
            XS[s] = (OWN[s] + CR[s].astype(F32)).astype(BF16)
            self.far = wires.send(XS.at[s], XR.at[self.stage, s], x_dev)

        def wait(self):
            self.far.wait_recv()

        def tile(self, r):
            at = pl.ds(r, TILE)
            return XS[self.s, at, :].astype(F32) + XR[self.stage, self.s, at, :].astype(F32)

    def feed_down(s):
        return Reduction(0, s, lambda rows: dot_nt(ACT[rows, :], WD[...]))

    zeros = jnp.zeros((8, D), F32)

    def norm_two(s, total):
        load_gout[s].wait()

        def body(r, carry):
            gain, shift, bias = carry
            rows = token_rows(s, r)
            second = total.tile(r) + vec(4) + NORMED[rows, :].astype(F32)
            xhat, scale = normalize(second)
            MIX[rows, :] = (xhat * vec(1) + vec(5)).astype(BF16)
            cot = GOUT[s, pl.ds(r, TILE), :].astype(F32)
            back = norm_back(cot * vec(1), xhat, scale)
            GS[s, pl.ds(r, TILE), :] = back
            low = back.astype(BF16)
            BR[rows, :] = low
            gain = gain + fold_rows(cot * xhat)
            shift = shift + fold_rows(cot)
            bias = bias + fold_rows(low.astype(F32))
            return gain, shift, bias

        add_small((1, 5, 4), tile_loop(half, body, (zeros, zeros, zeros)))
        return share(BR, s), share(MIX, s)

    def feed_back(s):
        def block(i, carry):
            start = s * L + i * CHUNK
            rows = pl.ds(pl.multiple_of(start, CHUNK), CHUNK)
            HB[...] = dot_nn(BR[rows, :], WD[...])

            def body(r, total):
                to = pl.ds(pl.multiple_of(start + r, TILE), TILE)
                low = (HB[pl.ds(r, TILE), :] * DG[to, :]).astype(BF16)
                GH[to, :] = low
                return total + fold_rows(low.astype(F32))

            return tile_loop(CHUNK, body, carry)

        sums = lax.fori_loop(0, L // CHUNK, block, jnp.zeros((8, FF), F32))
        SMG[10:11, :FF] += jnp.sum(sums, axis=0, keepdims=True)
        return Reduction(1, s, lambda rows: dot_nt(GH[rows, :], WU[...]))

    def norm_one_back(s, total):
        def body(r, carry):
            gain, shift, bias = carry
            at = pl.ds(r, TILE)
            cot = GS[s, at, :] + total.tile(r)
            xhat = XH1[s, at, :]
            back = norm_back(cot * vec(0), xhat, R1[s, at, 0:1])
            GS[s, at, :] = back
            low = back.astype(BF16)
            GAT[token_rows(s, r), :] = low
            gain = gain + fold_rows(cot * xhat)
            shift = shift + fold_rows(cot)
            bias = bias + fold_rows(low.astype(F32))
            return gain, shift, bias

        add_small((0, 3, 2), tile_loop(half, body, (zeros, zeros, zeros)))
        return share(GAT, s)

    def attend_back(s, between):
        base = s * L
        all_rows = slice(base, base + L)
        GC[...] = dot_nn(GAT[all_rows, :], outer[...]).astype(BF16)
        GQF[...] = jnp.zeros_like(GQF)
        GKF[...] = jnp.zeros_like(GKF)
        GVF[...] = jnp.zeros_like(GVF)
        load_gl[s].wait()

        for h in range(HEADS):
            pick, pick_v = head_mask(h), head_mask(h, PAIR - C)
            for b, (lo, hi) in enumerate(windows):
                rows = slice(b * EDGE, (b + 1) * EDGE)
                cot = GC[rows, :] * pick_v
                grad_prob = dot_nt(cot, V[base + lo : base + hi, :])
                prob_low = PROB[s, h, rows, : hi - lo]
                prob = prob_low.astype(F32)
                term = prob * grad_prob
                level = jnp.sum(term, axis=-1, keepdims=True)
                grad = term - prob * level + GLB[s, h, rows, lo:hi].astype(F32)
                GLB[s, h, rows, lo:hi] = grad.astype(BF16)
                GVF[lo:hi, :] += dot_tn(prob_low, cot)
            grad_raw = GLB[s, h]
            GQF[...] += dot_nn(grad_raw, K[all_rows, :] * pick)
            GKF[...] += dot_tn(grad_raw, Q[all_rows, :] * pick)
            for job in between[h]:
                job()
        low_q = (GQF[...] * 0.125).astype(BF16)
        low_k = (GKF[...] * 0.125).astype(BF16)
        low_v = GVF[...].astype(BF16)
        GP[all_rows, :EDGE] = low_q[:, :EDGE]
        GP[all_rows, EDGE:PAIR] = low_q[:, EDGE:] + low_v[:, :EDGE]
        GP[all_rows, PAIR : 3 * EDGE] = low_v[:, EDGE:]
        GP[all_rows, 3 * EDGE :] = low_k
        SMG[8:9, :PAIR] += jnp.sum(low_q.astype(F32), axis=0, keepdims=True)
        SMG[9:10, :PAIR] += jnp.sum(low_v.astype(F32), axis=0, keepdims=True)

        def product(rows):
            return dot_nt(GP[rows, :], WA[:, : 5 * EDGE])

        return Reduction(2, s, product)

    def token_grads(s, total):
        def body(r, carry):
            rows = token_rows(s, r)
            GT[rows, :] = (GS[s, pl.ds(r, TILE), :] + total.tile(r)).astype(BF16)
            return carry

        tile_loop(half, body, 0)
        return share(GT, s)

    class Scatter:
        def __init__(self, tag, fill):
            self.stage, self.yr = getattr(r_, "ST" + tag), getattr(r_, "YR" + tag)
            self.zs, self.zr = getattr(r_, "ZS" + tag), getattr(r_, "ZR" + tag)
            fill(self.stage)
            self.y_in = [
                wires.send(self.stage.at[1 - y, zto[k]], self.yr.at[zto[k]], y_dev)
                for k in range(1, Z)
            ]
            self.sent = []

        def late(self):
            self.last = wires.send(self.stage.at[1 - y, z], self.yr.at[z], y_dev)

        def block(self, index):
            return self.stage[y, index].astype(F32) + self.yr[index].astype(F32)

        def along(self, k):
            self.y_in[k - 1].wait_recv()
            self.zs[k - 1] = self.block(zto[k]).astype(BF16)
            self.sent.append(wires.send(self.zs.at[k - 1], self.zr.at[k - 1], z_dev[k]))

        def along_all(self):
            for k in range(1, Z):
                self.along(k)

        def finish(self):
            self.last.wait_recv()
            total = self.block(z)
            for k in range(1, Z):
                self.sent[k - 1].wait_recv()
                total = total + self.zr[k - 1].astype(F32)
            return total

    def fill_square(left, right):
        def fill(stage):
            part = D // 2
            for i in range(2):
                product = dot_tn(left[:, i * part : (i + 1) * part], right[...]).astype(BF16)
                for j in range(part // SH):
                    index = i * (part // SH) + j
                    stage[index % Y, index // Y] = product[j * SH : (j + 1) * SH, :]

        return fill

    def fill_blocks(stage, at, product):
        wide = product.shape[1]
        for index in range(Z * Y):
            stage[index % Y, index // Y, :, at : at + wide] = product[index * SH : (index + 1) * SH, :]

    def fill_first(stage):
        fill_blocks(stage, 0, dot_tn(tok[...], GP[:, : 3 * EDGE]).astype(BF16))

    def fill_second(stage):
        keys, outs = dot_tn(tok[...], GP[:, 3 * EDGE :]), r_.OG
        fill_blocks(stage, 0, keys[:, :EDGE].astype(BF16))
        fill_blocks(stage, EDGE, (keys[:, EDGE:] + outs[:, :EDGE]).astype(BF16))
        fill_blocks(stage, PAIR, outs[:, EDGE:].astype(BF16))

    def pass_on(gather, step):
        return lambda: gather.step(step)

    parts0 = attend(
        0,
        (
            (pass_on(gather_u, 2), gather_d.across),
            (gather_e.meet,),
            (pass_on(gather_d, 1),),
        ),
    )
    parts1 = attend(
        1,
        (
            (pass_on(gather_u, 3),),
            (pass_on(gather_d, 2), pass_on(gather_e, 1)),
            (),
        ),
    )
    wo_x.wait_recv()
    wo_d = wires.send(WO.at[1], WO.at[2], c_dev)
    gather_e.step(2)
    wo_core.wait_recv()
    wo_d.wait_recv()
    normed0 = out_project(0, parts0)
    gather_d.step(3)
    gather_u.finish()
    normed0.wait_recv()
    feed_up(0)
    gather_e.step(3)
    normed1 = out_project(1, parts1)
    gather_d.finish()
    down0 = feed_down(0)
    normed1.wait_recv()
    feed_up(1)
    down0.cross()
    down1 = feed_down(1)
    down0.wait()
    down1.cross()
    branch0, mix0 = norm_two(0, down0)
    branch0.wait_recv()
    back0 = feed_back(0)
    back0.cross()
    down1.wait()
    branch1, mix1 = norm_two(1, down1)
    branch1.wait_recv()
    scatter_d = Scatter("D", fill_square(BR, ACT))
    back1 = feed_back(1)
    scatter_u = Scatter("U", fill_square(NORMED, GH))
    scatter_d.along(1)
    back0.wait()
    back1.cross()
    attn0 = norm_one_back(0, back0)
    scatter_d.along(2)
    attn0.wait_recv()
    token0 = attend_back(0, ((), (), ()))
    token0.cross()
    scatter_d.along(3)
    back1.wait()
    attn1 = norm_one_back(1, back1)
    scatter_u.along(1)
    norms_core = wires.send(SMG.at[0:8], SMR.at[0], c_dev)
    attn1.wait_recv()
    r_.OG[...] = dot_tn(GAT[...], CTXF[...])
    norms_core.wait_recv()
    SMS[0] = SMG[0:8] + SMR[0]
    norms_y = wires.send(SMS.at[0], SMR.at[1], y_dev)
    scatter_d.late()
    scatter_u.late()

    def pass_up(step):
        return lambda: scatter_u.along(step)

    token1 = attend_back(1, ((), (pass_up(2),), (pass_up(3),)))
    heads_y = wires.send(SMG.at[8:16], SMR.at[5], y_dev)
    norms_y.wait_recv()
    SMS[1] = SMS[0] + SMR[1]
    norms_z = [wires.send(SMS.at[1], SMR.at[1 + k], z_dev[k]) for k in range(1, Z)]
    scatter_f = Scatter("F", fill_first)
    token0.wait()
    token1.cross()
    scatter_g = Scatter("G", fill_second)
    heads_y.wait_recv()
    SMS[2] = SMG[8:16] + SMR[5]
    heads_z = [wires.send(SMS.at[2], SMR.at[5 + k], z_dev[k]) for k in range(1, Z)]
    share0 = token_grads(0, token0)
    mix0.wait_recv()
    mix1.wait_recv()
    scatter_f.along_all()
    scatter_g.along_all()
    scatter_f.late()
    scatter_g.late()

    def collect(first, parts, into):
        value = first
        for k in range(1, Z):
            parts[k - 1].wait_recv()
            value = value + SMR[into + k]
        return value

    def own(value, count, width, start=0):
        mine_ = value[:count, start : start + width]
        for i in range(1, Z * Y):
            there = value[:count, start + i * width : start + (i + 1) * width]
            mine_ = jnp.where(dpi == i, there, mine_)
        return mine_

    token1.wait()
    share1 = token_grads(1, token1)
    norms = collect(SMS[1], norms_z, 1)
    r_.ggains[...] = own(norms, 2, SH)
    r_.gshifts[...] = own(norms[2:6], 4, SH)
    heads = collect(SMS[2], heads_z, 5)
    r_.ghbias[0:1] = own(heads[0:1], 1, piece)
    r_.ghbias[1:2] = own(heads[1:2], 1, piece, PAIR - C)
    r_.gfbias[...] = own(heads[2:3], 1, SH)
    r_.gd[...] = scatter_d.finish()
    r_.gu[...] = scatter_u.finish()
    share0.wait_recv()
    share1.wait_recv()
    first = scatter_f.finish()
    second = scatter_g.finish()
    r_.ga[0] = first[:, :C]
    r_.ga[2] = first[:, C:]
    r_.ga[1] = second[:, :C]
    r_.go[...] = jnp.transpose(second[:, C:])
    wires.drain_all()


def pass_kernel(count, *refs):
    sources, targets, sem = refs[:count], refs[count : 2 * count], refs[2 * count]
    stores = [
        pltpu.make_async_copy(sources[i], targets[i], sem.at[i]) for i in range(count)
    ]
    for copy in stores:
        copy.start()
    for copy in stores:
        copy.wait()


def pass_through(arrays):
    count = len(arrays)
    far = pl.BlockSpec(memory_space=pl.ANY)
    close = pl.BlockSpec(memory_space=pltpu.VMEM)
    return pl.pallas_call(
        functools.partial(pass_kernel, count),
        out_shape=tuple(jax.ShapeDtypeStruct(a.shape, a.dtype) for a in arrays),
        in_specs=[close] * count,
        out_specs=(far,) * count,
        scratch_shapes=[pltpu.SemaphoreType.DMA((count,))],
        compiler_params=pltpu.CompilerParams(vmem_limit_bytes=4 * 1024 * 1024),
    )(*arrays)


def fused_shards(
    tokens, segments, logits_in, w_qkv, w_out, w_up, w_down,
    head_bias, ff_bias, norm_gains, shift_biases, grad_out, grad_logits,
):
    rows, D = tokens.shape
    seqs, L = segments.shape
    HEADS = logits_in.shape[1]
    SH, unused, C = w_qkv.shape
    FF = w_up.shape[1]
    HD = C // HEADS
    half = L // 2
    width = max(D, FF)
    dma = pltpu.SemaphoreType.DMA
    vm = pltpu.VMEM
    inputs = dict(
        tok_far=tokens, wa_far=jnp.transpose(w_qkv, (1, 0, 2)), wo_far=w_out,
        wu=w_up, wd=w_down.T, hbias_far=head_bias, fbias_far=ff_bias[None],
        gains_far=norm_gains, shifts_far=shift_biases, seg_far=segments,
        gout=grad_out, lin=logits_in, gl=grad_logits,
    )
    outputs = dict(
        mixed=vm((rows, D), BF16),
        logits_out=vm(logits_in.shape, BF16),
        gtok=vm((rows, D), BF16),
        glin_out=vm(logits_in.shape, BF16),
        ga=vm((3, SH, C), F32),
        go=vm((C, SH), F32),
        gu=vm((SH, FF), F32),
        gd=vm((SH, FF), F32),
        ghbias=vm(head_bias.shape, F32),
        gfbias=vm((1,) + ff_bias.shape, F32),
        ggains=vm(norm_gains.shape, F32),
        gshifts=vm(shift_biases.shape, F32),
    )
    scratch = dict(
        tok=vm((rows, D), BF16), wa=vm((3, SH, C), BF16), wo=vm((C, SH), BF16),
        hbias=vm(head_bias.shape, BF16), fbias=vm((1,) + ff_bias.shape, BF16),
        gains=vm(norm_gains.shape, BF16), shifts=vm(shift_biases.shape, BF16),
        seg=vm(segments.shape, jnp.int32),
        WA=vm((D, 6 * EDGE), BF16), WU=vm((D, FF), BF16),
        WD=vm((D, FF), BF16), BLEND=vm((16, EDGE), F32),
        SM=vm((16, Z * Y * EDGE), BF16),
        SMV=vm((16, width), F32), HBV=vm((16, 4 * EDGE), F32), WO=vm((3, D, 2 * EDGE), BF16),
        GOUT=vm((seqs, half, D), BF16),
        Q=vm((rows, 2 * EDGE), BF16), K=vm((rows, 2 * EDGE), BF16), V=vm((rows, 2 * EDGE), BF16),

        PROB=vm((seqs, HEADS, L, 3 * EDGE), BF16), BIAS=vm((L, 3 * EDGE), F32),
        CTXF=vm((rows, 2 * EDGE), BF16), CTXR=vm((3, seqs, half, 2 * EDGE), BF16),
        NORMED=vm((rows, D), BF16), ACT=vm((rows, FF), BF16), DG=vm((rows, FF), F32),
        BR=vm((rows, D), BF16), GH=vm((rows, FF), BF16), GAT=vm((rows, D), BF16),
        GC=vm((L, 2 * EDGE), BF16),
        XH1=vm((seqs, half, D), F32), R1=vm((seqs, half, EDGE), F32),
        GS=vm((seqs, half, D), F32), HB=vm((CHUNK, width), F32),
        OWN=vm((seqs, half, D), F32), CS=vm((seqs, half, D), BF16),
        CR=vm((seqs, half, D), BF16), XS=vm((seqs, half, D), BF16),
        XR=vm((3, seqs, half, D), BF16), GP=vm((rows, 5 * EDGE), BF16), OG=vm((D, 2 * EDGE), F32),
        GQF=vm((L, 2 * EDGE), F32), GKF=vm((L, 2 * EDGE), F32), GVF=vm((L, 2 * EDGE), F32),
        SMG=vm((16, width), F32), SMS=vm((3, 8, width), F32), SMR=vm((9, 8, width), F32),
        send_sem=dma((SENDS,)), recv_sem=dma((ARRIVALS,)), local_sem=dma((LOADS,)),
    )
    for tag in "UDFG":
        block = (SH, FF if tag in "UD" else 3 * EDGE)
        scratch["ST" + tag] = vm((Y, Z) + block, BF16)
        scratch["YR" + tag] = vm((Z,) + block, BF16)
        scratch["ZS" + tag] = vm((Z - 1,) + block, BF16)
        scratch["ZR" + tag] = vm((Z - 1,) + block, BF16)
    far = pl.BlockSpec(memory_space=pl.ANY)
    close = pl.BlockSpec(memory_space=pltpu.VMEM)
    names = (*inputs, *outputs, *scratch)
    dims = (L, HEADS, HD, D, FF, C, SH)
    results = pl.pallas_call(
        functools.partial(layer_kernel, names, dims),
        out_shape=tuple(outputs.values()),
        in_specs=[far] * len(inputs),
        out_specs=(close,) * len(outputs),
        scratch_shapes=list(scratch.values()),
        compiler_params=pltpu.CompilerParams(
            collective_id=0, has_side_effects=True, vmem_limit_bytes=52 * 1024 * 1024
        ),
    )(*inputs.values())
    mixed, logits_out, gtok, glin, ga, go, gu, gd, ghbias, gfbias, ggains, gshifts = pass_through(
        results
    )
    return (
        mixed,
        logits_out,
        gtok,
        glin,
        jnp.transpose(ga, (1, 0, 2)),
        go,
        gu,
        gd.T,
        ghbias,
        gfbias[0],
        ggains,
        gshifts,
    )


def solution(mesh):
    body = fused_shards if mesh.shape["dp"] == Z * Y and mesh.shape["mp"] == 2 * CORES else shards
    return jax.shard_map(
        body,
        mesh=mesh,
        in_specs=(
            P("dp", None),
            P("dp", None),
            P("dp", "mp", None, None),
            P("dp", None, "mp"),
            P("mp", "dp"),
            P("dp", "mp"),
            P("mp", "dp"),
            P(None, ("mp", "dp")),
            P(("mp", "dp")),
            P(None, "dp"),
            P(None, "dp"),
            P("dp", None),
            P("dp", "mp", None, None),
        ),
        out_specs=(
            P("dp", None),
            P("dp", "mp", None, None),
            P("dp", None),
            P("dp", "mp", None, None),
            P("dp", None, "mp"),
            P("mp", "dp"),
            P("dp", "mp"),
            P("mp", "dp"),
            P(None, ("mp", "dp")),
            P(("mp", "dp")),
            P(None, "dp"),
            P(None, "dp"),
        ),
        check_vma=False,
    )
```

```python
import functools
import types

import jax
import jax.numpy as jnp
from jax import lax
from jax.experimental import pallas as pl
from jax.experimental.pallas import tpu as pltpu
from jax.sharding import PartitionSpec as P

MB = 2
MESH = pl.DeviceIdType.MESH
F32 = jnp.float32
BF16 = jnp.bfloat16

epsilon = 1e-05
masked_value = -10000.0


def norm_rows(hidden, gain, shift):
    center = hidden - jnp.mean(hidden, axis=-1, keepdims=True)
    spread = jnp.mean(center * center, axis=-1, keepdims=True)
    return center * lax.rsqrt(spread + epsilon) * gain + shift


def gelu_exact(value):
    return 0.5 * value * (1.0 + lax.erf(value * 0.7071067811865476))


def add_trees(first_tree, second_tree):
    if first_tree is None:
        return second_tree
    return jax.tree.map(jnp.add, first_tree, second_tree)


def micro_step(whole, block_tokens, block_segments, block_logits, block_grad, block_grad_logits):
    qkv_weight, out_weight, up_weight, down_weight, bias_heads, bias_hidden, gains, shifts = whole
    seq_count = block_segments.shape[0]
    length = block_segments.shape[1]
    feature = block_tokens.shape[1]
    row_count = block_tokens.shape[0]
    local_heads = block_logits.shape[1]
    flat_qkv = qkv_weight.reshape(feature, -1)
    local_cols = flat_qkv.shape[1] // 3
    head_size = local_cols // local_heads
    gain_rows = gains.astype(jnp.float32)
    shift_rows = shifts.astype(jnp.float32)
    head_rows = bias_heads.astype(jnp.float32)
    shape_heads = (seq_count, length, local_heads, head_size)
    token_float = block_tokens.astype(jnp.float32)
    projected = jnp.dot(block_tokens, flat_qkv, preferred_element_type=jnp.float32)
    query = (projected[:, :local_cols] + head_rows[0]).astype(jnp.bfloat16).reshape(shape_heads)
    keys = projected[:, local_cols : 2 * local_cols].astype(jnp.bfloat16).reshape(shape_heads)
    values = (
        (projected[:, 2 * local_cols :] + head_rows[1]).astype(jnp.bfloat16).reshape(shape_heads)
    )
    same = block_segments[:, :, None] == block_segments[:, None, :]
    mask = jnp.where(same, 0.0, masked_value).astype(jnp.float32)[:, None]
    incoming = block_logits.astype(jnp.float32)
    raw = (
        jnp.einsum("sqhd,skhd->shqk", query, keys, preferred_element_type=jnp.float32) * 0.125
        + incoming
    )
    shifted = raw + mask
    top = jnp.max(shifted, axis=-1, keepdims=True)
    expo = jnp.exp(shifted - top)
    total = jnp.sum(expo, axis=-1, keepdims=True)
    log_total = top + jnp.log(total)
    context = jnp.einsum(
        "shqk,skhd->sqhd",
        (expo / total).astype(jnp.bfloat16),
        values,
        preferred_element_type=jnp.float32,
    )
    context = context.reshape(row_count, local_cols).astype(jnp.bfloat16)
    attn_total = lax.psum(jnp.dot(context, out_weight, preferred_element_type=jnp.float32), "mp")
    first_pre = attn_total + shift_rows[0] + token_float
    normed = norm_rows(first_pre, gain_rows[0], shift_rows[1]).astype(jnp.bfloat16)
    hidden_pre = jnp.dot(
        normed, up_weight, preferred_element_type=jnp.float32
    ) + bias_hidden.astype(jnp.float32)
    activated = gelu_exact(hidden_pre).astype(jnp.bfloat16)
    ffn_total = lax.psum(jnp.dot(activated, down_weight, preferred_element_type=jnp.float32), "mp")
    second_pre = ffn_total + shift_rows[2] + normed.astype(jnp.float32)
    cotangent = block_grad.astype(jnp.float32)
    mixed_part = norm_rows(second_pre, gain_rows[1], shift_rows[3]).astype(jnp.bfloat16)
    unused_second, second_pull = jax.vjp(norm_rows, second_pre, gain_rows[1], shift_rows[3])
    grad_second, grad_gain_two, grad_shift_two = second_pull(cotangent)
    branch_part = grad_second.astype(jnp.bfloat16)
    grad_bias_two = jnp.sum(branch_part.astype(jnp.float32), axis=0)
    grad_down = jnp.einsum("rf,rd->fd", activated, branch_part, preferred_element_type=jnp.float32)
    grad_act = jnp.einsum("rd,fd->rf", branch_part, down_weight, preferred_element_type=jnp.float32)
    unused_gelu, gelu_pull = jax.vjp(gelu_exact, hidden_pre)
    grad_hidden = gelu_pull(grad_act)[0].astype(jnp.bfloat16)
    grad_bias_hidden = jnp.sum(grad_hidden.astype(jnp.float32), axis=0)
    grad_up = jnp.einsum("rd,rf->df", normed, grad_hidden, preferred_element_type=jnp.float32)
    hidden_terms = jnp.einsum(
        "rf,df->rd", grad_hidden, up_weight, preferred_element_type=jnp.float32
    )
    grad_normed = grad_second + lax.psum(hidden_terms, "mp")
    unused_first, first_pull = jax.vjp(norm_rows, first_pre, gain_rows[0], shift_rows[1])
    grad_first, grad_gain_one, grad_shift_one = first_pull(grad_normed)
    grad_attn = grad_first.astype(jnp.bfloat16)
    grad_bias_out = jnp.sum(grad_attn.astype(jnp.float32), axis=0)
    grad_out_weight = jnp.einsum(
        "rc,rd->cd", context, grad_attn, preferred_element_type=jnp.float32
    )
    grad_context = jnp.einsum(
        "rd,cd->rc", grad_attn, out_weight, preferred_element_type=jnp.float32
    )
    grad_context = grad_context.astype(jnp.bfloat16).reshape(shape_heads)
    raw_again = (
        jnp.einsum("sqhd,skhd->shqk", query, keys, preferred_element_type=jnp.float32) * 0.125
        + incoming
    )
    prob = jnp.exp(raw_again + mask - log_total)
    grad_prob = jnp.einsum(
        "sqhd,skhd->shqk", grad_context, values, preferred_element_type=jnp.float32
    )
    grad_raw = prob * (
        grad_prob - jnp.sum(prob * grad_prob, axis=-1, keepdims=True)
    ) + block_grad_logits.astype(jnp.float32)
    grad_raw_low = grad_raw.astype(jnp.bfloat16)
    grad_query = (
        jnp.einsum("shqk,skhd->sqhd", grad_raw_low, keys, preferred_element_type=jnp.float32)
        * 0.125
    )
    grad_keys = (
        jnp.einsum("shqk,sqhd->skhd", grad_raw_low, query, preferred_element_type=jnp.float32)
        * 0.125
    )
    grad_values = jnp.einsum(
        "shqk,sqhd->skhd",
        prob.astype(jnp.bfloat16),
        grad_context,
        preferred_element_type=jnp.float32,
    )
    grad_query = grad_query.astype(jnp.bfloat16).reshape(row_count, local_cols)
    grad_keys = grad_keys.astype(jnp.bfloat16).reshape(row_count, local_cols)
    grad_values = grad_values.astype(jnp.bfloat16).reshape(row_count, local_cols)
    grad_proj = jnp.concatenate([grad_query, grad_keys, grad_values], axis=1)
    grad_qkv = jnp.einsum(
        "rd,rc->dc", block_tokens, grad_proj, preferred_element_type=jnp.float32
    ).reshape(qkv_weight.shape)
    grad_heads = jnp.stack(
        [
            jnp.sum(grad_query.astype(jnp.float32), axis=0),
            jnp.sum(grad_values.astype(jnp.float32), axis=0),
        ]
    )
    input_terms = jnp.einsum("rc,dc->rd", grad_proj, flat_qkv, preferred_element_type=jnp.float32)
    grad_inputs = grad_first + lax.psum(input_terms.astype(jnp.bfloat16), "mp").astype(jnp.float32)
    results = (mixed_part, raw.astype(jnp.bfloat16), grad_inputs.astype(jnp.bfloat16), grad_raw_low)
    grads = (
        grad_qkv,
        grad_out_weight,
        grad_up,
        grad_down,
        grad_heads,
        grad_bias_hidden,
        jnp.stack([grad_gain_one, grad_gain_two]),
        jnp.stack([grad_bias_out, grad_shift_one, grad_bias_two, grad_shift_two]),
    )
    return (results, grads)


def shards(
    tokens,
    segments,
    logits_in,
    w_qkv,
    w_out,
    w_up,
    w_down,
    head_bias,
    ff_bias,
    norm_gains,
    shift_biases,
    grad_out,
    grad_logits,
):
    seq_count = segments.shape[0] // MB
    row_count = seq_count * segments.shape[1]
    collected = []
    totals = None
    for micro in range(MB):
        whole = (
            lax.all_gather(w_qkv, "dp", axis=0, tiled=True),
            lax.all_gather(w_out, "dp", axis=1, tiled=True),
            lax.all_gather(w_up, "dp", axis=0, tiled=True),
            lax.all_gather(w_down, "dp", axis=1, tiled=True),
            lax.all_gather(head_bias, "dp", axis=1, tiled=True),
            lax.all_gather(ff_bias, "dp", axis=0, tiled=True),
            lax.all_gather(norm_gains, "dp", axis=1, tiled=True),
            lax.all_gather(shift_biases, "dp", axis=1, tiled=True),
        )
        first_row = micro * row_count
        first_seq = micro * seq_count
        results, grads = micro_step(
            whole,
            tokens[first_row : first_row + row_count],
            segments[first_seq : first_seq + seq_count],
            logits_in[first_seq : first_seq + seq_count],
            grad_out[first_row : first_row + row_count],
            grad_logits[first_seq : first_seq + seq_count],
        )
        totals = add_trees(totals, grads)
        collected.append(results)
    totals = (
        lax.psum_scatter(totals[0], "dp", scatter_dimension=0, tiled=True),
        lax.psum_scatter(totals[1], "dp", scatter_dimension=1, tiled=True),
        lax.psum_scatter(totals[2], "dp", scatter_dimension=0, tiled=True),
        lax.psum_scatter(totals[3], "dp", scatter_dimension=1, tiled=True),
        lax.psum_scatter(totals[4], "dp", scatter_dimension=1, tiled=True),
        lax.psum_scatter(totals[5], "dp", scatter_dimension=0, tiled=True),
        lax.psum_scatter(totals[6], "dp", scatter_dimension=1, tiled=True),
        lax.psum_scatter(totals[7], "dp", scatter_dimension=1, tiled=True),
    )
    mixed = jnp.concatenate([item[0] for item in collected], axis=0)
    logits_out = jnp.concatenate([item[1] for item in collected], axis=0)
    grad_tokens = jnp.concatenate([item[2] for item in collected], axis=0)
    grad_logits_in = jnp.concatenate([item[3] for item in collected], axis=0)
    return (
        mixed,
        logits_out,
        grad_tokens,
        grad_logits_in,
        totals[0],
        totals[1],
        totals[2],
        totals[3],
        totals[4],
        totals[5],
        totals[6],
        totals[7],
    )


Z, Y, CORES = 4, 2, 2
TILE = 32
EDGE = 128
CHUNK = 256
SENDS, ARRIVALS, LOADS = 144, 116, 16


def dot_nn(a, b):
    return lax.dot_general(a, b, (((1,), (0,)), ((), ())), preferred_element_type=F32)


def dot_nt(a, b):
    return lax.dot_general(a, b, (((1,), (1,)), ((), ())), preferred_element_type=F32)


def dot_tn(a, b):
    return lax.dot_general(a, b, (((0,), (0,)), ((), ())), preferred_element_type=F32)


def fold_rows(value):
    rows, cols = value.shape
    return jnp.sum(value.reshape(rows // 8, 8, cols), axis=0)


class Wires:
    def __init__(self, send_sem, recv_sem):
        self.send_sem, self.recv_sem, self.sent, self.drained = send_sem, recv_sem, [], []
        self.slots = 0

    def take(self, count):
        self.slots += count
        return self.slots - count

    def describe(self, src, dst, device, out, into):
        return pltpu.make_async_remote_copy(
            src_ref=src,
            dst_ref=dst,
            send_sem=self.send_sem.at[out],
            recv_sem=self.recv_sem.at[into],
            device_id=device,
            device_id_type=MESH,
        )

    def send(self, src, dst, device, into=None):
        copy = self.describe(
            src, dst, device, len(self.sent), self.take(1) if into is None else into
        )
        copy.start()
        self.sent.append(copy)
        return copy

    def send_if(self, condition, src, dst, device, into):
        copy = self.describe(src, dst, device, len(self.sent), into)
        pl.when(condition)(copy.start)
        self.sent.append((copy, condition))

    def arrived(self, ref, device, into):
        self.describe(ref, ref, device, 0, into).wait_recv()

    def drain(self, copy):
        if not any(copy is done for done in self.drained):
            copy.wait_send()
            self.drained.append(copy)

    def drain_all(self):
        for copy in self.sent:
            if isinstance(copy, tuple):
                pl.when(copy[1])(copy[0].wait_send)
            elif not any(copy is done for done in self.drained):
                copy.wait_send()


def layer_kernel(names, dims, *refs):
    r_ = types.SimpleNamespace(**dict(zip(names, refs, strict=True)))
    L, HEADS, HD, D, FF, C, SH = dims
    seqs = 2
    half = L // 2
    tok, seg, GOUT = r_.tok, r_.seg, r_.GOUT
    WA, WU, WD, WO, SMV = r_.WA, r_.WU, r_.WD, r_.WO, r_.SMV
    Q, K, V, LIN, GLB, PROB = r_.Q, r_.K, r_.V, r_.logits_out, r_.glin_out, r_.PROB
    BIAS, CTXF, CTXR = r_.BIAS, r_.CTXF, r_.CTXR
    NORMED, ACT, DG, BR, GH, GAT = r_.NORMED, r_.ACT, r_.DG, r_.BR, r_.GH, r_.GAT
    GC, MIX, GT, XH1, R1, GS = r_.GC, r_.mixed, r_.gtok, r_.XH1, r_.R1, r_.GS
    HB, CS, CR, XS, XR = r_.HB, r_.CS, r_.CR, r_.XS, r_.XR
    OWN, GP = r_.OWN, r_.GP
    GQF, GKF, GVF = r_.GQF, r_.GKF, r_.GVF
    SMG, SMS, SMR = r_.SMG, r_.SMS, r_.SMR
    local_sem = r_.local_sem

    dpi, mpi = lax.axis_index("dp"), lax.axis_index("mp")
    z, y = lax.div(dpi, Y), lax.rem(dpi, Y)
    x, core = lax.div(mpi, CORES), lax.rem(mpi, CORES)
    wires = Wires(r_.send_sem, r_.recv_sem)

    def dev(zz, yy, xx, cc):
        return {"dp": zz * Y + yy, "mp": xx * CORES + cc}

    zto = [lax.rem(z + k, Z) for k in range(Z)]
    zfrom = [lax.rem(z - k + Z, Z) for k in range(Z)]
    z_dev = [dev(zto[k], y, x, core) for k in range(Z)]
    y_dev = dev(z, 1 - y, x, core)
    c_dev = dev(z, y, x, 1 - core)
    x_dev = dev(z, y, 1 - x, core)
    d_dev = dev(z, y, 1 - x, 1 - core)

    barrier = pltpu.get_barrier_semaphore()
    friends = z_dev[1:] + [y_dev, c_dev, x_dev, d_dev]
    for friend in friends:
        pl.semaphore_signal(barrier, inc=1, device_id=friend, device_id_type=MESH)

    locals_used = []

    def local(src, dst):
        copy = pltpu.make_async_copy(src, dst, local_sem.at[len(locals_used)])
        copy.start()
        locals_used.append(copy)
        return copy

    def rows_of(index):
        return pl.ds(pl.multiple_of(index * SH, SH), SH)

    load_first = [local(r_.wa_far, r_.wa), local(r_.wo_far, r_.wo)]
    load_vecs = [
        local(r_.hbias_far, r_.hbias),
        local(r_.fbias_far, r_.fbias),
        local(r_.gains_far, r_.gains),
        local(r_.shifts_far, r_.shifts),
    ]
    load_up = local(r_.wu, WU.at[rows_of(dpi), :])
    load_down = local(r_.wd, WD.at[rows_of(dpi), :])
    load_tok = local(r_.tok_far, tok)
    load_seg = local(r_.seg_far, seg)
    load_lin = [local(r_.lin.at[s], LIN.at[s]) for s in range(seqs)]
    load_gout = [
        local(
            r_.gout.at[pl.ds(pl.multiple_of(s * L + core * half, half), half), :],
            GOUT.at[s],
        )
        for s in range(seqs)
    ]
    load_gl = [local(r_.gl.at[s], GLB.at[s]) for s in range(seqs)]
    def iotas(rows, cols):
        down = lax.broadcasted_iota(jnp.int32, (rows, cols), 0)
        return down, lax.broadcasted_iota(jnp.int32, (rows, cols), 1)

    def shifted(rows, cols, by):
        down, over = iotas(rows, cols)
        return jnp.where(over - down == by, 1.0, 0.0).astype(BF16)

    PAIR = 2 * EDGE
    wa, here = r_.wa, rows_of(dpi)
    even, odd = shifted(C, PAIR, 0), shifted(C, PAIR, PAIR - C)
    for copy in load_first:
        copy.wait()
    out_low = dot_nt(shifted(SH, SH, 0), r_.wo[...]).astype(BF16)
    for at, first, second in ((0, wa[0], wa[2]), (3 * EDGE, wa[1], out_low)):
        first, second = dot_nn(first, even), dot_nn(second, odd)
        WA[here, at : at + EDGE] = first[:, :EDGE].astype(BF16)
        WA[here, at + EDGE : at + PAIR] = (first[:, EDGE:] + second[:, :EDGE]).astype(BF16)
        WA[here, at + PAIR : at + 3 * EDGE] = second[:, EDGE:].astype(BF16)

    pl.semaphore_wait(barrier, len(friends))

    near = z - 1 + 2 * lax.div(3 - z, 3)
    last = 3 * (1 - lax.div(z, 2))
    order = [near, 6 - z - near - last, last]

    class Gather:
        def __init__(self, dst, place):
            self.dst, self.place = dst, place
            self.own = dst.at[place(dpi)]
            self.z_in, self.y_in = wires.take(Z), wires.take(Z)

        def along(self):
            for there in order:
                wires.send(self.own, self.own, dev(there, y, x, core), self.z_in + z)

        def across(self):
            wires.send(self.own, self.own, y_dev, self.y_in + z)

        def forward(self, step):
            origin = order[step]
            block = self.dst.at[self.place(origin * Y + y)]
            wires.arrived(block, y_dev, self.z_in + origin)
            wires.send(block, block, y_dev, self.y_in + origin)

        def finish(self):
            for origin in range(Z):
                block = self.dst.at[self.place(origin * Y + 1 - y)]
                wires.arrived(block, y_dev, self.y_in + origin)

    class Line(Gather):
        turns = True

        def block(self, origin):
            return self.dst.at[self.place(jnp.clip(origin, 0, Z - 1) * Y + y)]

        def push(self, src, origin, held, side):
            block = self.block(origin)
            room, there = ((z < Z - 1, z + 1), (z > 0, z - 1))[side]
            going = room if held is None else jnp.logical_and(room, held)
            device = dev(jnp.clip(there, 0, Z - 1), y, x, core)
            slot = self.z_in + jnp.clip(origin, 0, Z - 1)
            wires.send_if(going, src, block, device, slot)

        def start(self):
            for side in range(2):
                self.push(self.own, z, None, side)

        def step(self, hop):
            for side, origin, held in ((0, z - hop, z >= hop), (1, z + hop, z + hop < Z)):
                block = self.block(origin)
                slot = jnp.clip(origin, 0, Z - 1)

                @pl.when(held)
                def arrive():
                    wires.arrived(block, y_dev, self.z_in + slot)

                self.push(block, origin, held, side)
                if self.turns:
                    wires.send_if(held, block, block, y_dev, self.y_in + slot)

    class PairLine(Line):
        turns = False

        def __init__(self, dst, place, place_pair):
            Gather.__init__(self, dst, place)
            self.place_pair = place_pair

        def block(self, origin):
            return self.dst.at[self.place_pair(jnp.clip(origin, 0, Z - 1))]

        def meet(self):
            wires.arrived(self.dst.at[self.place(z * Y + 1 - y)], y_dev, self.y_in + z)
            self.own = self.block(z)
            self.start()

    def rows_of(index):
        return pl.ds(pl.multiple_of(index * SH, SH), SH)

    def lanes_of(start, stop):
        return lambda index: (rows_of(index), slice(start, stop))

    def by_lanes(index):
        return (slice(None), pl.ds(pl.multiple_of(index * EDGE, EDGE), EDGE))

    SM = r_.SM
    gather_a = Line(WA, lanes_of(0, 3 * EDGE))
    gather_b = Line(WA, lanes_of(3 * EDGE, 6 * EDGE))
    gather_s = Gather(SM, by_lanes)
    gather_u = Line(WU, lanes_of(0, FF))
    cut = FF - PAIR
    gather_d = Line(WD, lanes_of(0, cut))
    gather_e = PairLine(
        WD,
        lanes_of(cut, FF),
        lambda i: (pl.ds(pl.multiple_of(i * Y * SH, Y * SH), Y * SH), slice(cut, FF)),
    )

    gather_a.start()
    gather_b.start()
    gather_a.across()
    gather_b.across()

    for copy in load_vecs:
        copy.wait()
    blend = r_.BLEND
    blend[...] = jnp.zeros_like(blend)
    blend[0:2, :SH] = r_.gains[...].astype(F32)
    blend[2:6, :SH] = r_.shifts[...].astype(F32)
    piece = r_.hbias.shape[1]
    blend[8:10, :piece] = r_.hbias[...].astype(F32)
    blend[10:11, :SH] = r_.fbias[...].astype(F32)
    SM[by_lanes(dpi)] = blend[...].astype(BF16)
    gather_s.along()
    gather_s.across()
    gather_a.step(1)
    gather_b.step(1)
    for i in range(Z * Y):
        rows = slice(i * EDGE, (i + 1) * EDGE)
        down, over = iotas(EDGE, GH.shape[1])
        GH[rows, :] = jnp.where((over - down == i * SH) & (down < SH), 1.0, 0.0).astype(BF16)
        down, over = iotas(EDGE, 2 * PAIR)
        gap = i * piece + jnp.where(over < PAIR, 0, PAIR + PAIR - C)
        ACT[rows, : 2 * PAIR] = jnp.where(
            (over - down == gap) & (down < piece), 1.0, 0.0
        ).astype(BF16)

    gather_a.step(2)
    gather_b.step(2)
    gather_a.step(3)
    gather_b.step(3)
    load_up.wait()
    load_down.wait()
    gather_u.start()
    for step in range(Z - 1):
        gather_s.forward(step)
    gather_a.finish()
    gather_b.finish()
    gather_s.finish()
    gather_u.across()
    gather_e.across()
    outer = WA.at[:, 4 * EDGE : 6 * EDGE]
    wo_core = wires.send(outer, WO.at[0], c_dev)
    wo_x = wires.send(outer, WO.at[1], x_dev)

    SMV[...] = dot_nn(SM[...], GH[...])
    r_.HBV[...] = dot_nn(SM[...], ACT[:, : 2 * PAIR])
    SMG[...] = jnp.zeros_like(SMG)

    def vec(row, width=D):
        return SMV[row : row + 1, :width]

    def project(i, carry):
        rows = pl.ds(pl.multiple_of(i * CHUNK, CHUNK), CHUNK)
        block = tok[rows, :]
        HBV = r_.HBV
        Q[rows, :] = (dot_nn(block, WA[:, :PAIR]) + HBV[8:9, :PAIR]).astype(BF16)
        V[rows, :] = (dot_nn(block, WA[:, EDGE : 3 * EDGE]) + HBV[9:10, PAIR:]).astype(BF16)
        K[rows, :] = dot_nn(block, WA[:, 3 * EDGE : 5 * EDGE]).astype(BF16)
        return carry

    gather_u.step(1)
    gather_d.start()
    load_tok.wait()
    load_seg.wait()
    lax.fori_loop(0, seqs * L // CHUNK, project, 0)

    lanes = lax.broadcasted_iota(jnp.int32, (1, PAIR), 1)

    def head_mask(h, start=0):
        inside = (lanes >= start + h * HD) & (lanes < start + (h + 1) * HD)
        return jnp.where(inside, 1.0, 0.0).astype(BF16)

    blocks = L // EDGE
    windows = [(max(b - 1, 0) * EDGE, min(b + 2, blocks) * EDGE) for b in range(blocks)]

    def half_of(s, which):
        return pl.ds(pl.multiple_of(s * L + which * half, half), half)

    def mine(s):
        return half_of(s, core)

    def theirs(s):
        return half_of(s, 1 - core)

    def attend(s, between):
        base = s * L
        ids = seg[s : s + 1, :].astype(F32)
        tall = jnp.transpose(jnp.broadcast_to(ids, (EDGE, L)))
        for b, (lo, hi) in enumerate(windows):
            for j in range((hi - lo) // EDGE):
                near = ids[:, lo + j * EDGE : lo + (j + 1) * EDGE]
                same = tall[b * EDGE : (b + 1) * EDGE, :] == near
                BIAS[b * EDGE : (b + 1) * EDGE, j * EDGE : (j + 1) * EDGE] = jnp.where(
                    same, 0.0, masked_value
                ).astype(F32)
        GQF[...] = jnp.zeros_like(GQF)
        load_lin[s].wait()

        for h in range(HEADS):
            pick, pick_v = head_mask(h), head_mask(h, PAIR - C)
            for b, (lo, hi) in enumerate(windows):
                rows = slice(b * EDGE, (b + 1) * EDGE)
                query = Q[base + b * EDGE : base + (b + 1) * EDGE, :] * pick
                score = dot_nt(query, K[base : base + L, :])
                raw = score * 0.125 + LIN[s, h, rows, :].astype(F32)
                LIN[s, h, rows, :] = raw.astype(BF16)
                near = raw[:, lo:hi] + BIAS[rows, : hi - lo]
                top = jnp.max(near, axis=-1, keepdims=True)
                expo = jnp.exp(near - top)
                norm = 1.0 / jnp.sum(expo, axis=-1, keepdims=True)
                prob = (expo * norm).astype(BF16)
                PROB[s, h, rows, : hi - lo] = prob
                GQF[rows, :] += dot_nn(prob, V[base + lo : base + hi, :] * pick_v)
            for job in between[h]:
                job()
        CTXF[base : base + L, :] = GQF[...].astype(BF16)
        parts = [
            wires.send(CTXF.at[theirs(s), :], CTXR.at[0, s], c_dev),
            wires.send(CTXF.at[mine(s), :], CTXR.at[1, s], x_dev),
            wires.send(CTXF.at[theirs(s), :], CTXR.at[2, s], d_dev),
        ]
        return parts

    def tile_loop(count, body, init):
        def step(i, carry):
            start = pl.multiple_of(i * 2 * TILE, 2 * TILE)
            return body(start + TILE, body(start, carry))

        return lax.fori_loop(0, count // (2 * TILE), step, init)

    def token_rows(s, r):
        return pl.ds(pl.multiple_of(s * L + core * half + r, TILE), TILE)

    def normalize(value):
        center = value - jnp.mean(value, axis=-1, keepdims=True)
        spread = jnp.mean(center * center, axis=-1, keepdims=True)
        scale = lax.rsqrt(spread + epsilon)
        return center * scale, scale

    def norm_back(scaled, xhat, scale):
        flat = jnp.mean(scaled, axis=-1, keepdims=True)
        tilt = jnp.mean(scaled * xhat, axis=-1, keepdims=True)
        return scale * (scaled - flat - xhat * tilt)

    def add_small(rows, sums):
        for row, value in zip(rows, sums, strict=True):
            SMG[row : row + 1, :] += jnp.sum(value, axis=0, keepdims=True)

    def share(ref, s):
        return wires.send(ref.at[mine(s), :], ref.at[mine(s), :], c_dev)

    def out_project(s, parts):
        for copy in parts:
            copy.wait_recv()
        HB[...] = dot_nt(CTXF[mine(s), :], outer[...]) + dot_nt(CTXR[0, s], WO[0])
        OWN[s] = dot_nt(CTXR[1, s], WO[1]) + dot_nt(CTXR[2, s], WO[2])

        def body(r, carry):
            at = pl.ds(r, TILE)
            first = (HB[at, :] + OWN[s, at, :]) + vec(2) + tok[token_rows(s, r), :].astype(F32)
            xhat, scale = normalize(first)
            XH1[s, at, :] = xhat
            R1[s, at, :] = jnp.broadcast_to(scale, (TILE, EDGE))
            NORMED[token_rows(s, r), :] = (xhat * vec(0) + vec(3)).astype(BF16)
            return carry

        tile_loop(half, body, 0)
        return share(NORMED, s)

    def feed_up(s):
        def block(i, carry):
            start = s * L + i * CHUNK
            rows = pl.ds(pl.multiple_of(start, CHUNK), CHUNK)
            HB[...] = dot_nn(NORMED[rows, :], WU[...]) + vec(10, FF)

            def body(r, inner):
                to = pl.ds(pl.multiple_of(start + r, TILE), TILE)
                value = HB[pl.ds(r, TILE), :]
                cdf = 0.5 * (1.0 + lax.erf(value * 0.7071067811865476))
                ACT[to, :] = (value * cdf).astype(BF16)
                DG[to, :] = cdf + value * (jnp.exp(-0.5 * value * value) * 0.3989422804014327)
                return inner

            return tile_loop(CHUNK, body, carry)

        lax.fori_loop(0, L // CHUNK, block, 0)

    last_sum = [None] * seqs

    class Reduction:
        def __init__(self, stage, s, product):
            self.stage, self.s = stage, s
            before = last_sum[s]
            if before is not None:
                wires.drain(before.pair)
                wires.drain(before.far)
            last_sum[s] = self
            CS[s] = product(theirs(s)).astype(BF16)
            self.pair = wires.send(CS.at[s], CR.at[s], c_dev)
            OWN[s] = product(mine(s))

        def cross(self):
            s = self.s
            self.pair.wait_recv()
            XS[s] = (OWN[s] + CR[s].astype(F32)).astype(BF16)
            self.far = wires.send(XS.at[s], XR.at[self.stage, s], x_dev)

        def wait(self):
            self.far.wait_recv()

        def tile(self, r):
            at = pl.ds(r, TILE)
            return XS[self.s, at, :].astype(F32) + XR[self.stage, self.s, at, :].astype(F32)

    def feed_down(s):
        return Reduction(0, s, lambda rows: dot_nt(ACT[rows, :], WD[...]))

    zeros = jnp.zeros((8, D), F32)

    def norm_two(s, total):
        load_gout[s].wait()

        def body(r, carry):
            gain, shift, bias = carry
            rows = token_rows(s, r)
            second = total.tile(r) + vec(4) + NORMED[rows, :].astype(F32)
            xhat, scale = normalize(second)
            MIX[rows, :] = (xhat * vec(1) + vec(5)).astype(BF16)
            cot = GOUT[s, pl.ds(r, TILE), :].astype(F32)
            back = norm_back(cot * vec(1), xhat, scale)
            GS[s, pl.ds(r, TILE), :] = back
            low = back.astype(BF16)
            BR[rows, :] = low
            gain = gain + fold_rows(cot * xhat)
            shift = shift + fold_rows(cot)
            bias = bias + fold_rows(low.astype(F32))
            return gain, shift, bias

        add_small((1, 5, 4), tile_loop(half, body, (zeros, zeros, zeros)))
        return share(BR, s), share(MIX, s)

    def feed_back(s):
        def block(i, carry):
            start = s * L + i * CHUNK
            rows = pl.ds(pl.multiple_of(start, CHUNK), CHUNK)
            HB[...] = dot_nn(BR[rows, :], WD[...])

            def body(r, total):
                to = pl.ds(pl.multiple_of(start + r, TILE), TILE)
                low = (HB[pl.ds(r, TILE), :] * DG[to, :]).astype(BF16)
                GH[to, :] = low
                return total + fold_rows(low.astype(F32))

            return tile_loop(CHUNK, body, carry)

        sums = lax.fori_loop(0, L // CHUNK, block, jnp.zeros((8, FF), F32))
        SMG[10:11, :FF] += jnp.sum(sums, axis=0, keepdims=True)
        return Reduction(1, s, lambda rows: dot_nt(GH[rows, :], WU[...]))

    def norm_one_back(s, total):
        def body(r, carry):
            gain, shift, bias = carry
            at = pl.ds(r, TILE)
            cot = GS[s, at, :] + total.tile(r)
            xhat = XH1[s, at, :]
            back = norm_back(cot * vec(0), xhat, R1[s, at, 0:1])
            GS[s, at, :] = back
            low = back.astype(BF16)
            GAT[token_rows(s, r), :] = low
            gain = gain + fold_rows(cot * xhat)
            shift = shift + fold_rows(cot)
            bias = bias + fold_rows(low.astype(F32))
            return gain, shift, bias

        add_small((0, 3, 2), tile_loop(half, body, (zeros, zeros, zeros)))
        return share(GAT, s)

    def attend_back(s, between):
        base = s * L
        all_rows = slice(base, base + L)
        GC[...] = dot_nn(GAT[all_rows, :], outer[...]).astype(BF16)
        GQF[...] = jnp.zeros_like(GQF)
        GKF[...] = jnp.zeros_like(GKF)
        GVF[...] = jnp.zeros_like(GVF)
        load_gl[s].wait()

        for h in range(HEADS):
            pick, pick_v = head_mask(h), head_mask(h, PAIR - C)
            for b, (lo, hi) in enumerate(windows):
                rows = slice(b * EDGE, (b + 1) * EDGE)
                cot = GC[rows, :] * pick_v
                grad_prob = dot_nt(cot, V[base + lo : base + hi, :])
                prob_low = PROB[s, h, rows, : hi - lo]
                prob = prob_low.astype(F32)
                term = prob * grad_prob
                level = jnp.sum(term, axis=-1, keepdims=True)
                grad = term - prob * level + GLB[s, h, rows, lo:hi].astype(F32)
                GLB[s, h, rows, lo:hi] = grad.astype(BF16)
                GVF[lo:hi, :] += dot_tn(prob_low, cot)
            grad_raw = GLB[s, h]
            GQF[...] += dot_nn(grad_raw, K[all_rows, :] * pick)
            GKF[...] += dot_tn(grad_raw, Q[all_rows, :] * pick)
            for job in between[h]:
                job()
        low_q = (GQF[...] * 0.125).astype(BF16)
        low_k = (GKF[...] * 0.125).astype(BF16)
        low_v = GVF[...].astype(BF16)
        GP[all_rows, :EDGE] = low_q[:, :EDGE]
        GP[all_rows, EDGE:PAIR] = low_q[:, EDGE:] + low_v[:, :EDGE]
        GP[all_rows, PAIR : 3 * EDGE] = low_v[:, EDGE:]
        GP[all_rows, 3 * EDGE :] = low_k
        SMG[8:9, :PAIR] += jnp.sum(low_q.astype(F32), axis=0, keepdims=True)
        SMG[9:10, :PAIR] += jnp.sum(low_v.astype(F32), axis=0, keepdims=True)

        def product(rows):
            return dot_nt(GP[rows, :], WA[:, : 5 * EDGE])

        return Reduction(2, s, product)

    def token_grads(s, total):
        def body(r, carry):
            rows = token_rows(s, r)
            GT[rows, :] = (GS[s, pl.ds(r, TILE), :] + total.tile(r)).astype(BF16)
            return carry

        tile_loop(half, body, 0)
        return share(GT, s)

    class Scatter:
        def __init__(self, tag, fill):
            self.stage, self.yr = getattr(r_, "ST" + tag), getattr(r_, "YR" + tag)
            self.zs, self.zr = getattr(r_, "ZS" + tag), getattr(r_, "ZR" + tag)
            fill(self.stage)
            self.y_in = [
                wires.send(self.stage.at[1 - y, zto[k]], self.yr.at[zto[k]], y_dev)
                for k in range(1, Z)
            ]
            self.sent = []

        def late(self):
            self.last = wires.send(self.stage.at[1 - y, z], self.yr.at[z], y_dev)

        def block(self, index):
            return self.stage[y, index].astype(F32) + self.yr[index].astype(F32)

        def along(self, k):
            self.y_in[k - 1].wait_recv()
            self.zs[k - 1] = self.block(zto[k]).astype(BF16)
            self.sent.append(wires.send(self.zs.at[k - 1], self.zr.at[k - 1], z_dev[k]))

        def along_all(self):
            for k in range(1, Z):
                self.along(k)

        def finish(self):
            self.last.wait_recv()
            total = self.block(z)
            for k in range(1, Z):
                self.sent[k - 1].wait_recv()
                total = total + self.zr[k - 1].astype(F32)
            return total

    def fill_square(left, right):
        def fill(stage):
            part = D // 2
            for i in range(2):
                product = dot_tn(left[:, i * part : (i + 1) * part], right[...]).astype(BF16)
                for j in range(part // SH):
                    index = i * (part // SH) + j
                    stage[index % Y, index // Y] = product[j * SH : (j + 1) * SH, :]

        return fill

    def fill_blocks(stage, at, product):
        wide = product.shape[1]
        for index in range(Z * Y):
            stage[index % Y, index // Y, :, at : at + wide] = product[index * SH : (index + 1) * SH, :]

    def fill_first(stage):
        fill_blocks(stage, 0, dot_tn(tok[...], GP[:, : 3 * EDGE]).astype(BF16))

    def fill_second(stage):
        keys, outs = dot_tn(tok[...], GP[:, 3 * EDGE :]), r_.OG
        fill_blocks(stage, 0, keys[:, :EDGE].astype(BF16))
        fill_blocks(stage, EDGE, (keys[:, EDGE:] + outs[:, :EDGE]).astype(BF16))
        fill_blocks(stage, PAIR, outs[:, EDGE:].astype(BF16))

    def pass_on(gather, step):
        return lambda: gather.step(step)

    parts0 = attend(
        0,
        (
            (gather_d.across,),
            (pass_on(gather_u, 2), gather_e.meet),
            (pass_on(gather_d, 1),),
        ),
    )
    parts1 = attend(1, ((pass_on(gather_u, 3),), (), (pass_on(gather_d, 2),)))
    wo_x.wait_recv()
    wo_d = wires.send(WO.at[1], WO.at[2], c_dev)
    wo_core.wait_recv()
    wo_d.wait_recv()
    normed0 = out_project(0, parts0)
    gather_e.step(1)
    gather_u.finish()
    normed0.wait_recv()
    gather_d.step(3)
    feed_up(0)
    gather_e.step(2)
    normed1 = out_project(1, parts1)
    gather_e.step(3)
    gather_d.finish()
    down0 = feed_down(0)
    normed1.wait_recv()
    feed_up(1)
    down0.cross()
    down1 = feed_down(1)
    wires.drain(down0.far)
    down1.cross()
    down0.wait()
    branch0, mix0 = norm_two(0, down0)
    branch0.wait_recv()
    back0 = feed_back(0)
    back0.cross()
    down1.wait()
    branch1, mix1 = norm_two(1, down1)
    branch1.wait_recv()
    scatter_d = Scatter("D", fill_square(BR, ACT))
    back1 = feed_back(1)
    scatter_u = Scatter("U", fill_square(NORMED, GH))
    back1.cross()
    scatter_d.along(1)
    back0.wait()
    attn0 = norm_one_back(0, back0)
    scatter_d.along(2)
    attn0.wait_recv()
    token0 = attend_back(0, ((), (), ()))
    scatter_d.along(3)
    back1.wait()
    attn1 = norm_one_back(1, back1)
    token0.cross()
    scatter_u.along(1)
    norms_core = wires.send(SMG.at[0:8], SMR.at[0], c_dev)
    attn1.wait_recv()
    r_.OG[...] = dot_tn(GAT[...], CTXF[...])
    norms_core.wait_recv()
    SMS[0] = SMG[0:8] + SMR[0]
    norms_y = wires.send(SMS.at[0], SMR.at[1], y_dev)
    scatter_d.late()

    def pass_up(step):
        return lambda: scatter_u.along(step)

    token1 = attend_back(1, ((), (pass_up(2),), (pass_up(3),)))
    heads_y = wires.send(SMG.at[8:16], SMR.at[5], y_dev)
    scatter_f = Scatter("F", fill_first)
    norms_y.wait_recv()
    SMS[1] = SMS[0] + SMR[1]
    norms_z = [wires.send(SMS.at[1], SMR.at[1 + k], z_dev[k]) for k in range(1, Z)]
    token1.cross()
    scatter_g = Scatter("G", fill_second)
    heads_y.wait_recv()
    SMS[2] = SMG[8:16] + SMR[5]
    heads_z = [wires.send(SMS.at[2], SMR.at[5 + k], z_dev[k]) for k in range(1, Z)]
    token0.wait()
    share0 = token_grads(0, token0)
    mix0.wait_recv()
    mix1.wait_recv()
    scatter_f.along_all()
    scatter_g.along_all()
    scatter_u.late()
    scatter_f.late()
    scatter_g.late()

    def collect(first, parts, into):
        value = first
        for k in range(1, Z):
            parts[k - 1].wait_recv()
            value = value + SMR[into + k]
        return value

    def own(value, count, width, start=0):
        mine_ = value[:count, start : start + width]
        for i in range(1, Z * Y):
            there = value[:count, start + i * width : start + (i + 1) * width]
            mine_ = jnp.where(dpi == i, there, mine_)
        return mine_

    token1.wait()
    share1 = token_grads(1, token1)
    norms = collect(SMS[1], norms_z, 1)
    r_.ggains[...] = own(norms, 2, SH)
    r_.gshifts[...] = own(norms[2:6], 4, SH)
    heads = collect(SMS[2], heads_z, 5)
    r_.ghbias[0:1] = own(heads[0:1], 1, piece)
    r_.ghbias[1:2] = own(heads[1:2], 1, piece, PAIR - C)
    r_.gfbias[...] = own(heads[2:3], 1, SH)
    r_.gd[...] = scatter_d.finish()
    r_.gu[...] = scatter_u.finish()
    share0.wait_recv()
    share1.wait_recv()
    first = scatter_f.finish()
    second = scatter_g.finish()
    r_.ga[0] = first[:, :C]
    r_.ga[2] = first[:, C:]
    r_.ga[1] = second[:, :C]
    r_.go[...] = jnp.transpose(second[:, C:])
    wires.drain_all()


def pass_kernel(count, *refs):
    sources, targets, sem = refs[:count], refs[count : 2 * count], refs[2 * count]
    stores = [
        pltpu.make_async_copy(sources[i], targets[i], sem.at[i]) for i in range(count)
    ]
    for copy in stores:
        copy.start()
    for copy in stores:
        copy.wait()


def pass_through(arrays):
    count = len(arrays)
    far = pl.BlockSpec(memory_space=pl.ANY)
    close = pl.BlockSpec(memory_space=pltpu.VMEM)
    return pl.pallas_call(
        functools.partial(pass_kernel, count),
        out_shape=tuple(jax.ShapeDtypeStruct(a.shape, a.dtype) for a in arrays),
        in_specs=[close] * count,
        out_specs=(far,) * count,
        scratch_shapes=[pltpu.SemaphoreType.DMA((count,))],
        compiler_params=pltpu.CompilerParams(vmem_limit_bytes=4 * 1024 * 1024),
    )(*arrays)


def fused_shards(
    tokens, segments, logits_in, w_qkv, w_out, w_up, w_down,
    head_bias, ff_bias, norm_gains, shift_biases, grad_out, grad_logits,
):
    rows, D = tokens.shape
    seqs, L = segments.shape
    HEADS = logits_in.shape[1]
    SH, unused, C = w_qkv.shape
    FF = w_up.shape[1]
    HD = C // HEADS
    half = L // 2
    width = max(D, FF)
    dma = pltpu.SemaphoreType.DMA
    vm = pltpu.VMEM
    inputs = dict(
        tok_far=tokens, wa_far=jnp.transpose(w_qkv, (1, 0, 2)), wo_far=w_out,
        wu=w_up, wd=w_down.T, hbias_far=head_bias, fbias_far=ff_bias[None],
        gains_far=norm_gains, shifts_far=shift_biases, seg_far=segments,
        gout=grad_out, lin=logits_in, gl=grad_logits,
    )
    outputs = dict(
        mixed=vm((rows, D), BF16),
        logits_out=vm(logits_in.shape, BF16),
        gtok=vm((rows, D), BF16),
        glin_out=vm(logits_in.shape, BF16),
        ga=vm((3, SH, C), F32),
        go=vm((C, SH), F32),
        gu=vm((SH, FF), F32),
        gd=vm((SH, FF), F32),
        ghbias=vm(head_bias.shape, F32),
        gfbias=vm((1,) + ff_bias.shape, F32),
        ggains=vm(norm_gains.shape, F32),
        gshifts=vm(shift_biases.shape, F32),
    )
    scratch = dict(
        tok=vm((rows, D), BF16), wa=vm((3, SH, C), BF16), wo=vm((C, SH), BF16),
        hbias=vm(head_bias.shape, BF16), fbias=vm((1,) + ff_bias.shape, BF16),
        gains=vm(norm_gains.shape, BF16), shifts=vm(shift_biases.shape, BF16),
        seg=vm(segments.shape, jnp.int32),
        WA=vm((D, 6 * EDGE), BF16), WU=vm((D, FF), BF16),
        WD=vm((D, FF), BF16), BLEND=vm((16, EDGE), F32),
        SM=vm((16, Z * Y * EDGE), BF16),
        SMV=vm((16, width), F32), HBV=vm((16, 4 * EDGE), F32), WO=vm((3, D, 2 * EDGE), BF16),
        GOUT=vm((seqs, half, D), BF16),
        Q=vm((rows, 2 * EDGE), BF16), K=vm((rows, 2 * EDGE), BF16), V=vm((rows, 2 * EDGE), BF16),

        PROB=vm((seqs, HEADS, L, 3 * EDGE), BF16), BIAS=vm((L, 3 * EDGE), F32),
        CTXF=vm((rows, 2 * EDGE), BF16), CTXR=vm((3, seqs, half, 2 * EDGE), BF16),
        NORMED=vm((rows, D), BF16), ACT=vm((rows, FF), BF16), DG=vm((rows, FF), F32),
        BR=vm((rows, D), BF16), GH=vm((rows, FF), BF16), GAT=vm((rows, D), BF16),
        GC=vm((L, 2 * EDGE), BF16),
        XH1=vm((seqs, half, D), F32), R1=vm((seqs, half, EDGE), F32),
        GS=vm((seqs, half, D), F32), HB=vm((CHUNK, width), F32),
        OWN=vm((seqs, half, D), F32), CS=vm((seqs, half, D), BF16),
        CR=vm((seqs, half, D), BF16), XS=vm((seqs, half, D), BF16),
        XR=vm((3, seqs, half, D), BF16), GP=vm((rows, 5 * EDGE), BF16), OG=vm((D, 2 * EDGE), F32),
        GQF=vm((L, 2 * EDGE), F32), GKF=vm((L, 2 * EDGE), F32), GVF=vm((L, 2 * EDGE), F32),
        SMG=vm((16, width), F32), SMS=vm((3, 8, width), F32), SMR=vm((9, 8, width), F32),
        send_sem=dma((SENDS,)), recv_sem=dma((ARRIVALS,)), local_sem=dma((LOADS,)),
    )
    for tag in "UDFG":
        block = (SH, FF if tag in "UD" else 3 * EDGE)
        scratch["ST" + tag] = vm((Y, Z) + block, BF16)
        scratch["YR" + tag] = vm((Z,) + block, BF16)
        scratch["ZS" + tag] = vm((Z - 1,) + block, BF16)
        scratch["ZR" + tag] = vm((Z - 1,) + block, BF16)
    far = pl.BlockSpec(memory_space=pl.ANY)
    close = pl.BlockSpec(memory_space=pltpu.VMEM)
    names = (*inputs, *outputs, *scratch)
    dims = (L, HEADS, HD, D, FF, C, SH)
    results = pl.pallas_call(
        functools.partial(layer_kernel, names, dims),
        out_shape=tuple(outputs.values()),
        in_specs=[far] * len(inputs),
        out_specs=(close,) * len(outputs),
        scratch_shapes=list(scratch.values()),
        compiler_params=pltpu.CompilerParams(
            collective_id=0, has_side_effects=True, vmem_limit_bytes=52 * 1024 * 1024
        ),
    )(*inputs.values())
    mixed, logits_out, gtok, glin, ga, go, gu, gd, ghbias, gfbias, ggains, gshifts = pass_through(
        results
    )
    return (
        mixed,
        logits_out,
        gtok,
        glin,
        jnp.transpose(ga, (1, 0, 2)),
        go,
        gu,
        gd.T,
        ghbias,
        gfbias[0],
        ggains,
        gshifts,
    )


def solution(mesh):
    body = fused_shards if mesh.shape["dp"] == Z * Y and mesh.shape["mp"] == 2 * CORES else shards
    return jax.shard_map(
        body,
        mesh=mesh,
        in_specs=(
            P("dp", None),
            P("dp", None),
            P("dp", "mp", None, None),
            P("dp", None, "mp"),
            P("mp", "dp"),
            P("dp", "mp"),
            P("mp", "dp"),
            P(None, ("mp", "dp")),
            P(("mp", "dp")),
            P(None, "dp"),
            P(None, "dp"),
            P("dp", None),
            P("dp", "mp", None, None),
        ),
        out_specs=(
            P("dp", None),
            P("dp", "mp", None, None),
            P("dp", None),
            P("dp", "mp", None, None),
            P("dp", None, "mp"),
            P("mp", "dp"),
            P("dp", "mp"),
            P("mp", "dp"),
            P(None, ("mp", "dp")),
            P(("mp", "dp")),
            P(None, "dp"),
            P(None, "dp"),
        ),
        check_vma=False,
    )
```
